256 devices in a mesh: dp: 64 (over z, y, core), comp: 4 (over x).
Axes of the slice: x: 4, y: 4, z: 8, core: 2. Of those that a mesh axis runs over, the one named last changes fastest.
Arguments:
- points: float32 [65536, 128], P('dp'), may hold values from -64 to 64
- block_counts: int32 [64], replicated, may hold values from 1 to 16, as said below
- block_dest: int32 [64, 16], replicated, may hold values from 0 to 63, as said below
- means: float32 [256, 128], P(('dp', 'comp')), may hold values from -3 to 3
- factors: float32 [256, 128, 128], P(('dp', 'comp')), may hold values from -0.25 to 1.4, as said below
- log_weights: float32 [256], P(('dp', 'comp')), may hold values from -4 to 4
Outputs:
- new_means: float32 [256, 128], P(('dp', 'comp'))
- new_factors: float32 [256, 128, 128], P(('dp', 'comp'))
- new_log_weights: float32 [256], P(('dp', 'comp'))
- log_density: float32 [16384], P('dp')
The draws below stay inside these ranges and needn't reach their ends.
Inputs may be any that keep to these rules, and one draw needn't show every extreme that they name: `block_counts`: blocks live on each index of dp on entry; they sum to 256, and one index holds exactly 16. `block_dest`: for j < block_counts[s], the index of dp that receives block j of index s; every index receives exactly 4 blocks, no index sends more than 1 block to one index, and some index sends exactly 1 to one; entries with j >= block_counts[s] are unused. `factors`: each matrix is upper triangular with diagonal entries from 0.7 to 1.4.
All inputs are finite; a program needn't handle non-finite values.
Results may differ from the reference program's by a relative error of at most 0.003.
Values sent between devices are 32-bit elements; how exact they have to be, the bound alone decides.
A program may use at most 128 MiB of HBM per device.

```python
import math
import jax
import jax.numpy as jnp
from jax import lax

D = 128
K = 256
BR = 64
RB = 4
ITERS = 2
NB = 16
N_DP = 64


def layout_tables(key):
    base_key = jax.random.fold_in(key, 7)
    key_hot, key_moves, key_perm = jax.random.split(base_key, 3)
    hottest = jax.random.randint(key_hot, (), 0, N_DP).astype(jnp.int32)
    counts = jnp.full((N_DP,), RB, jnp.int32)
    device_ids = jnp.arange(N_DP, dtype=jnp.int32)

    def lift(turn_index, current):
        others = jnp.where(device_ids == hottest, -1, current)
        donor_index = jnp.argmax(others).astype(jnp.int32)
        amount = (current[hottest] < NB).astype(jnp.int32)
        return current.at[donor_index].add(-amount).at[hottest].add(amount)
    counts = lax.fori_loop(0, NB, lift, counts)
    move_total = 8 * N_DP * RB
    move_pairs = jax.random.randint(key_moves, (move_total, 2), 0, N_DP).astype(jnp.int32)

    def wander(turn_index, current):
        donor_index = move_pairs[turn_index, 0]
        taker_index = move_pairs[turn_index, 1]
        allowed = (current[donor_index] > 1) & (current[taker_index] < NB - 1) & (donor_index != taker_index)
        allowed = allowed & (donor_index != hottest) & (taker_index != hottest)
        amount = allowed.astype(jnp.int32)
        return current.at[donor_index].add(-amount).at[taker_index].add(amount)
    counts = lax.fori_loop(0, move_total, wander, counts)
    positions = jnp.arange(NB, dtype=jnp.int32)
    prefix = jnp.cumsum(counts).astype(jnp.int32) - counts
    order_index = prefix[:, None] + positions[None, :]
    shuffle = jax.random.permutation(key_perm, N_DP).astype(jnp.int32)
    return (counts, shuffle[order_index % N_DP])


def draw_block_counts(key, part):
    return layout_tables(key)[0]


def draw_block_dest(key, part):
    return layout_tables(key)[1]


def draw_points(key, part):
    base_draw = jnp.clip(jax.random.normal(key, (N_DP * NB * BR, D), jnp.float32), -6.0, 6.0)
    return base_draw


def draw_factors(key, part):
    diag_key = jax.random.fold_in(key, 11)
    off_key = jax.random.fold_in(key, 13)
    diagonal = jax.random.uniform(diag_key, (K, D), jnp.float32, 0.7, 1.4)
    spread = jnp.clip(jax.random.normal(off_key, (K, D, D), jnp.float32), -4.0, 4.0) * (0.35 / D ** 0.5)
    return jnp.triu(spread, 1) + diagonal[:, :, None] * jnp.eye(D, dtype=jnp.float32)


def level_of(rng, shape, shards, smallest, high):
    def one(axis_at, blocks):
        steps = jax.random.uniform(jax.random.fold_in(jax.random.fold_in(rng, 6), axis_at), (blocks,), jnp.float32, smallest / len(shards), high / len(shards))
        return jnp.repeat(jnp.exp(steps), shape[axis_at] // blocks).reshape((-1,) + (1,) * (len(shape) - axis_at - 1))

    gain = one(*shards[0])
    for cut in shards[1:]:
        gain = gain * one(*cut)
    return gain


def noise(key, extent, width, reach, pieces=(), kind=jnp.bfloat16):
    drawn = width * jax.random.normal(key, extent, jnp.float32)
    if pieces:
        drawn = drawn * level_of(key, extent, pieces, -0.22, 0.18)
    return jnp.clip(drawn, -reach, reach).astype(kind)


def setup_inputs(seed: int = 0) -> dict:
    keys = jax.random.split(jax.random.key(seed), 7)
    points = draw_points(jax.random.fold_in(keys[6], 71), 0)
    block_counts = draw_block_counts(jax.random.fold_in(keys[6], 71), 0)
    block_dest = draw_block_dest(jax.random.fold_in(keys[6], 71), 0)
    means = noise(keys[3], (K, D), 0.5, 3.0, ((0, 256),), jnp.float32)
    factors = draw_factors(jax.random.fold_in(keys[6], 71), 0)
    log_weights = noise(keys[5], (K,), 1.0, 4.0, ((0, 256),), jnp.float32)
    return dict(points=points, block_counts=block_counts, block_dest=block_dest, means=means, factors=factors, log_weights=log_weights)


highest = lax.Precision.HIGHEST
ridge_term = 1.0
log_two_pi = math.log(2.0 * math.pi)

def rebalance(points, block_counts, block_dest):
    blocks = points.reshape(N_DP * NB, BR, D)
    positions = jnp.arange(NB, dtype=jnp.int32)
    live_flag = (positions[None, :] < block_counts[:, None]).reshape(-1)
    targets = block_dest.reshape(-1).astype(jnp.int32)
    devices = jnp.arange(N_DP, dtype=jnp.int32)
    target_hits = ((targets[:, None] == devices[None, :]) & live_flag[:, None]).astype(jnp.int32)
    earlier = jnp.cumsum(target_hits, axis=0).astype(jnp.int32) - target_hits
    block_rank = jnp.sum(earlier * target_hits, axis=1).astype(jnp.int32)
    places = jnp.where(live_flag, targets * RB + block_rank, N_DP * RB).astype(jnp.int32)
    placed = jnp.zeros((N_DP * RB, BR, D), jnp.float32).at[places].set(blocks, mode='drop')
    return placed.reshape(N_DP * RB * BR, D)

def component_density(points_live, centres, factor_set, weights):

    def single(inputs):
        centre, factor, weight = inputs
        projected = jnp.dot(points_live - centre[None, :], factor, precision=highest)
        logdet = jnp.sum(jnp.log(jnp.diagonal(factor)))
        return weight + logdet - 0.5 * D * log_two_pi - 0.5 * jnp.sum(projected * projected, axis=1)
    return lax.map(single, (centres, factor_set, weights))

def moments(points_live, centres, responsibility):

    def single(inputs):
        centre, weight_row = inputs
        shifted = points_live - centre[None, :]
        weight_sum = jnp.sum(weight_row)
        first_moment = jnp.dot(weight_row, shifted, precision=highest)
        second_moment = lax.dot_general(shifted * weight_row[:, None], shifted, (((0,), (0,)), ((), ())), precision=highest)
        return (weight_sum, first_moment, second_moment)
    return lax.map(single, (centres, responsibility))

def refresh(centres, weight_sum, first_moment, second_moment, total_points):
    identity = jnp.eye(centres.shape[1], dtype=jnp.float32)
    counted = weight_sum + 1.0
    covariance = (second_moment - first_moment[:, :, None] * first_moment[:, None, :] / counted[:, None, None] + ridge_term * identity) / counted[:, None, None]
    cholesky_lower = jnp.linalg.cholesky(covariance)
    inverse_lower = jax.scipy.linalg.solve_triangular(cholesky_lower, jnp.broadcast_to(identity, covariance.shape), lower=True)
    return (centres + first_moment / counted[:, None], jnp.swapaxes(inverse_lower, 1, 2), jnp.log(counted / total_points))

def reference(points, block_counts, block_dest, means, factors, log_weights):
    points_live = rebalance(points, block_counts, block_dest)
    total_points = float(N_DP * RB * BR + K)
    centres, factor_set, weights = (means, factors, log_weights)
    log_total = jnp.zeros((N_DP * RB * BR,), jnp.float32)
    for iteration in range(ITERS):
        log_table = component_density(points_live, centres, factor_set, weights)
        row_peak = jnp.max(log_table, axis=0)
        log_total = row_peak + jnp.log(jnp.sum(jnp.exp(log_table - row_peak[None, :]), axis=0))
        responsibility = jnp.exp(log_table - log_total[None, :])
        weight_sum, first_moment, second_moment = moments(points_live, centres, responsibility)
        centres, factor_set, weights = refresh(centres, weight_sum, first_moment, second_moment, total_points)
    return (centres, factor_set, weights, log_total / D)
```

```python
import math

import jax
import jax.numpy as jnp
from jax import lax
from jax.experimental import pallas as pl
from jax.experimental.pallas import tpu as pltpu
from jax.sharding import Mesh
from jax.sharding import PartitionSpec as P

D = 128
BR = 64
RB = 4
ITERS = 2
Z, Y, C, X = "dp_0", "dp_1", "dp_2", "comp"
DP = (Z, Y, C)
DP_COMP = (Z, Y, C, X)
NZ, NY, NC, NX = 8, 4, 2, 4
NPTS = NZ * NY * NC * NX * BR
ROWS = NPTS // D
RA, RB_, RC = 24, 24, 16
BASE_B = NZ * NY * NC * NX * RA
BASE_C = BASE_B + NZ * NY * NC * NX * RB_
CHUNK = 1024
LOG_TWO_PI = math.log(2.0 * math.pi)
MESH = pl.DeviceIdType.MESH
F32, BF16 = jnp.float32, jnp.bfloat16
VMEM_LIMIT = 60 * 1024 * 1024


def vmem():
    return pl.BlockSpec(memory_space=pltpu.VMEM)


def smem():
    return pl.BlockSpec(memory_space=pltpu.SMEM)


def here():
    return lax.axis_index(Z), lax.axis_index(Y), lax.axis_index(C), lax.axis_index(X)


def shifted(place, step, size):
    return lax.rem(place + (step + size), size)


def offset_a(k, x, y=0, z=0):
    return (((k * NX + x) * NY + y) * NZ + z) * RA


def offset_b(k, y, z=0, x=0):
    return BASE_B + (((k * NY + y) * NZ + z) * NX + x) * RB_


def offset_c(k, z, x=0, y=0):
    return BASE_C + (((k * NZ + z) * NX + x) * NY + y) * RC


def gather_kernel(
    from_slot, own_slot, slots, out, r1, s2, r2,
    send1, recv1, send2, recv2, sendg, recvg, sends, recvs, sendk, recvk,
):
    z, y, k, x = here()
    side = y * NC + k
    nside = NY * NC

    def side_of(step):
        t = shifted(side, step, nside)
        return {Y: t // NC, C: lax.rem(t, NC)}

    barrier = pltpu.get_barrier_semaphore()
    for step in range(1, nside):
        pl.semaphore_signal(barrier, inc=1, device_id=side_of(step), device_id_type=MESH)
    for step in range(1, NZ):
        pl.semaphore_signal(
            barrier, inc=1, device_id={Z: shifted(z, step, NZ)}, device_id_type=MESH
        )
    for step in range(1, NX):
        pl.semaphore_signal(
            barrier, inc=1, device_id={X: shifted(x, step, NX)}, device_id_type=MESH
        )
    pl.semaphore_wait(barrier, nside - 1 + NZ - 1 + NX - 1)

    def remote(src, dst, ssem, rsem, target):
        return pltpu.make_async_remote_copy(
            src_ref=src, dst_ref=dst, send_sem=ssem, recv_sem=rsem,
            device_id=target, device_id_type=MESH,
        )

    copies = []
    for step in range(1, nside):
        t = shifted(side, step, nside)
        copies.append(
            remote(slots.at[t], r1.at[side], send1.at[step], recv1.at[step], side_of(step))
        )
        copies[-1].start()
    r1[side] = slots[side]
    for copy in copies:
        copy.wait()
    for t in range(NZ):
        s2[t] = r1[from_slot[t]]
    copies = []
    for step in range(1, NZ):
        t = shifted(z, step, NZ)
        copies.append(remote(s2.at[t], r2.at[z], send2.at[step], recv2.at[step], {Z: t}))
        copies[-1].start()
    r2[z] = s2[z]
    for copy in copies:
        copy.wait()
    block = r2[own_slot[0]]

    def rows(start, size):
        return out.at[pl.ds(pl.multiple_of(start, 8), size)]

    rows(offset_a(k, x, y, z), RA)[...] = block[:RA]
    rows(offset_b(k, y, z, x), RB_)[...] = block[RA : RA + RB_]
    rows(offset_c(k, z, x, y), RC)[...] = block[RA + RB_ :]

    number = 0
    stages = (
        (
            (Z, z, NZ, offset_a(k, x, y, z), RA),
            (X, x, NX, offset_b(k, y, z, x), RB_),
            (Y, y, NY, offset_c(k, z, x, y), RC),
        ),
        (
            (Z, z, NZ, offset_b(k, y, z), NX * RB_),
            (Y, y, NY, offset_a(k, x, y), NZ * RA),
            (X, x, NX, offset_c(k, z, x), NY * RC),
        ),
    )
    for stage in stages:
        copies = []
        for axis, place, size, start, count in stage:
            part = rows(start, count)
            for step in range(1, size):
                copies.append(
                    remote(
                        part, part, sendg.at[number], recvg.at[number],
                        {axis: shifted(place, step, size)},
                    )
                )
                copies[-1].start()
                number += 1
        for copy in copies:
            copy.wait()

    other = {C: 1 - k}
    rings = (
        (X, x, NX, lambda at: offset_a(k, at), NY * NZ * RA),
        (Y, y, NY, lambda at: offset_b(k, at), NZ * NX * RB_),
        (Z, z, NZ, lambda at: offset_c(k, at), NX * NY * RC),
    )
    pieces = {}
    waiting = []
    to_other = []
    number = 0

    def pass_on(start, size):
        part = rows(start, size)
        n = len(to_other)
        to_other.append(remote(part, part, sendk.at[n], recvk.at[n], other))
        to_other[-1].start()

    def half_start(start, size, half):
        return start + half * (size // 2)

    def send(ring, way, step, half):
        axis, place, size, start_of, unit = rings[ring]
        start = half_start(start_of(shifted(place, -way * (step - 1), size)), unit, half)
        part = rows(start, unit // 2)
        n = len(waiting)
        copy = remote(
            part, part, sends.at[n], recvs.at[n], {axis: shifted(place, way, size)}
        )
        copy.start()
        waiting.append(copy)
        pieces[ring, way, step, half] = copy

    order = []
    for ring in (0, 1, 2):
        steps = rings[ring][2] // 2
        for step in range(1, steps + 1):
            for late in (0, 1):
                if step == steps and late:
                    continue
                scale = 2.8 if ring < 2 else 1.0
                for way in (1, -1):
                    half = late if way == 1 else 1 - late
                    order.append((scale * (2 * step + late - 1), ring, way, step, half))
    order.sort(key=lambda row: row[0])
    for _, ring, way, step, half in order:
        if step == 1:
            send(ring, way, step, half)
    for axis, place, size, start_of, unit in rings:
        pass_on(start_of(place), unit)
    for _, ring, way, step, half in order:
        axis, place, size, start_of, unit = rings[ring]
        pieces[ring, way, step, half].wait_recv()
        steps = size // 2
        if step + 1 < steps or (step + 1 == steps and half == (0 if way == 1 else 1)):
            send(ring, way, step + 1, half)
        start = half_start(start_of(shifted(place, -way * step, size)), unit, half)
        pass_on(start, unit // 2)
    for copy in waiting:
        copy.wait_send()
    for copy in to_other:
        copy.wait()


N_DIRECT = 2 * (NZ - 1) + 2 * (NX - 1) + 2 * (NY - 1)
N_RING = 2 * (NX - 1) + 2 * (NY - 1) + 2 * (NZ - 1)
N_OTHER = N_RING + 3


def gathered_points(slots, from_slot, own_slot):
    sem = pltpu.SemaphoreType.DMA
    nside = NY * NC
    return pl.pallas_call(
        gather_kernel,
        out_shape=jax.ShapeDtypeStruct((NPTS, D), F32),
        in_specs=[smem(), smem(), vmem()],
        out_specs=vmem(),
        scratch_shapes=[
            pltpu.VMEM((nside, BR, D), F32),
            pltpu.VMEM((NZ, BR, D), F32),
            pltpu.VMEM((NZ, BR, D), F32),
            sem((nside,)), sem((nside,)), sem((NZ,)), sem((NZ,)),
            sem((N_DIRECT,)), sem((N_DIRECT,)),
            sem((N_RING,)), sem((N_RING,)),
            sem((N_OTHER,)), sem((N_OTHER,)),
        ],
        compiler_params=pltpu.CompilerParams(
            collective_id=0, has_side_effects=True, vmem_limit_bytes=VMEM_LIMIT
        ),
        name="gather_points",
    )(from_slot, own_slot, slots)


def live_slots(points, block_counts):
    z, y, k, x = here()
    s = (z * NY + y) * NC + k
    prefix = jnp.cumsum(block_counts) - block_counts
    blocks = points.reshape(-1, BR, D)
    group = NY * NC * NX
    slot = jnp.arange(NY * NC, dtype=jnp.int32) * NX + x
    block = jnp.bitwise_and(slot - prefix[s], group - 1)
    picked = jnp.take(blocks, jnp.minimum(block, blocks.shape[0] - 1), axis=0)
    mine = (y * NC + k) * NX + x
    senders = z * NY * NC + jnp.arange(NY * NC, dtype=jnp.int32)
    j = jnp.bitwise_and(mine - prefix[senders], group - 1)
    live = j < block_counts[senders]
    to_z = (prefix[senders] + j) // group
    targets = jnp.arange(NZ, dtype=jnp.int32)
    hit = ((to_z[None, :] == targets[:, None]) & live[None, :]).astype(jnp.int32)
    from_slot = jnp.sum(hit * jnp.arange(NY * NC, dtype=jnp.int32)[None, :], axis=1)
    own = z * group + mine
    first = jnp.sum((prefix <= own).astype(jnp.int32)) - 1
    own_slot = (first // (NY * NC)).reshape(1)
    return picked, from_slot.astype(jnp.int32), own_slot.astype(jnp.int32)


def lse_kernel(
    table, out, r0, v, rx, u, ry, w, rz,
    send0, recv0, sendx, recvx, sendy, recvy, sendz, recvz, sendo, recvo, sendk, recvk,
):
    z, y, k, x = here()
    other = {C: 1 - k}
    barrier = pltpu.get_barrier_semaphore()
    pl.semaphore_signal(barrier, inc=1, device_id=other, device_id_type=MESH)
    for axis, place, size in ((X, x, NX), (Y, y, NY), (Z, z, NZ)):
        for step in range(1, size):
            pl.semaphore_signal(
                barrier, inc=1, device_id={axis: shifted(place, step, size)},
                device_id_type=MESH,
            )
    pl.semaphore_wait(barrier, 1 + NX - 1 + NY - 1 + NZ - 1)

    def remote(src, dst, ssem, rsem, target):
        return pltpu.make_async_remote_copy(
            src_ref=src, dst_ref=dst, send_sem=ssem, recv_sem=rsem,
            device_id=target, device_id_type=MESH,
        )

    def joined(parts):
        peak = parts[0]
        for part in parts[1:]:
            peak = jnp.maximum(peak, part)
        total = jnp.exp(parts[0] - peak)
        for part in parts[1:]:
            total = total + jnp.exp(part - peak)
        return peak + jnp.log(total)

    copy = remote(table.at[1 - k], r0, send0, recv0, other)
    copy.start()
    copy.wait()
    v[...] = joined([table[k], r0[...]])
    copies = []
    for step in range(1, NX):
        t = shifted(x, step, NX)
        copies.append(
            remote(v.at[t], rx.at[step - 1], sendx.at[step], recvx.at[step], {X: t})
        )
        copies[-1].start()
    for copy in copies:
        copy.wait()
    u[...] = joined([v[x]] + [rx[i] for i in range(NX - 1)])
    copies = []
    for step in range(1, NY):
        copies.append(
            remote(
                u, ry.at[step - 1], sendy.at[step], recvy.at[step], {Y: shifted(y, step, NY)}
            )
        )
        copies[-1].start()
    for copy in copies:
        copy.wait()
    w[...] = joined([u[...]] + [ry[i] for i in range(NY - 1)])
    copies = []
    for step in range(1, NZ):
        copies.append(
            remote(
                w, rz.at[step - 1], sendz.at[step], recvz.at[step], {Z: shifted(z, step, NZ)}
            )
        )
        copies[-1].start()
    for copy in copies:
        copy.wait()
    out[k, x] = joined([w[...]] + [rz[i] for i in range(NZ - 1)])
    copies = []
    for step in range(1, NX):
        part = out.at[k, x]
        copies.append(
            remote(part, part, sendo.at[step], recvo.at[step], {X: shifted(x, step, NX)})
        )
        copies[-1].start()
    to_other = []
    part = out.at[k, x]
    to_other.append(remote(part, part, sendk.at[0], recvk.at[0], other))
    to_other[-1].start()
    for step in range(1, NX):
        copies[step - 1].wait()
        part = out.at[k, shifted(x, -step, NX)]
        to_other.append(remote(part, part, sendk.at[step], recvk.at[step], other))
        to_other[-1].start()
    for copy in to_other:
        copy.wait()


def log_totals(table):
    sem = pltpu.SemaphoreType.DMA
    piece = ROWS // (NC * NX)
    total = pl.pallas_call(
        lse_kernel,
        out_shape=jax.ShapeDtypeStruct((NC, NX, piece, D), F32),
        in_specs=[vmem()],
        out_specs=vmem(),
        scratch_shapes=[
            pltpu.VMEM((NX, piece, D), F32),
            pltpu.VMEM((NX, piece, D), F32),
            pltpu.VMEM((NX - 1, piece, D), F32),
            pltpu.VMEM((piece, D), F32),
            pltpu.VMEM((NY - 1, piece, D), F32),
            pltpu.VMEM((piece, D), F32),
            pltpu.VMEM((NZ - 1, piece, D), F32),
            sem, sem,
            sem((NX,)), sem((NX,)), sem((NY,)), sem((NY,)), sem((NZ,)), sem((NZ,)),
            sem((NX,)), sem((NX,)), sem((NX,)), sem((NX,)),
        ],
        compiler_params=pltpu.CompilerParams(collective_id=1, has_side_effects=True),
        name="log_totals",
    )(table.reshape(NC, NX, piece, D))
    return total.reshape(ROWS, D)


def split2(value):
    high = value.astype(BF16)
    return high, (value - high.astype(F32)).astype(BF16)


def split3(value):
    high = value.astype(BF16)
    rest = value - high.astype(F32)
    middle = rest.astype(BF16)
    return high, middle, (rest - middle.astype(F32)).astype(BF16)


def dot(a, b):
    return jnp.dot(a, b, preferred_element_type=F32)


def eye():
    return (
        lax.broadcasted_iota(jnp.int32, (D, D), 0) == lax.broadcasted_iota(jnp.int32, (D, D), 1)
    ).astype(F32)


def spread(row):
    return jnp.transpose(jnp.broadcast_to(row, (D, D)))


def density(xt_ref, table_ref, mean, factor, weight):
    turned = jnp.transpose(factor)
    high, middle, low = split3(turned)
    main = jnp.concatenate(
        [jnp.concatenate([high, high], axis=1), jnp.concatenate([middle, middle], axis=1)], axis=0
    )
    rest = jnp.concatenate([high, low], axis=1)
    diagonal = jnp.sum(factor * eye(), axis=0, keepdims=True)
    offset = (
        weight + jnp.sum(jnp.log(diagonal), axis=1, keepdims=True) - 0.5 * D * LOG_TWO_PI
    )
    centre = spread(mean)
    groups = CHUNK // D

    def step(i, carry):
        start = pl.multiple_of(i * CHUNK, CHUNK)
        shift = xt_ref[:, pl.ds(start, CHUNK)] - jnp.concatenate([centre] * groups, axis=1)
        a, b, c = split3(shift)
        both = dot(main, jnp.concatenate([a, b], axis=0))
        value = both[:D] + both[D:] + dot(rest, jnp.concatenate([c, a], axis=0))
        row = offset - 0.5 * jnp.sum(value * value, axis=0, keepdims=True)
        for g in range(groups):
            table_ref[pl.ds(i * groups + g, 1), :] = row[:, g * D : (g + 1) * D]
        return carry

    lax.fori_loop(0, NPTS // CHUNK, step, 0)


def turn_points(x_ref, xt_ref):
    def step(i, carry):
        start = pl.multiple_of(i * CHUNK, CHUNK)
        xt_ref[:, pl.ds(start, CHUNK)] = jnp.transpose(x_ref[pl.ds(start, CHUNK), :])
        return carry

    lax.fori_loop(0, NPTS // CHUNK, step, 0)


def first_density_kernel(x_ref, mean_ref, factor_ref, weight_ref, xt_ref, table_ref):
    turn_points(x_ref, xt_ref)
    density(xt_ref, table_ref, mean_ref[...], factor_ref[...], weight_ref[...])


def moments(x_ref, xt_ref, table_ref, total_ref, mean, acc):
    centre = spread(mean)
    groups = CHUNK // D
    acc[...] = jnp.zeros_like(acc)

    def step(i, carry):
        first, count = carry
        start = pl.multiple_of(i * CHUNK, CHUNK)
        at = pl.multiple_of(i * groups, groups)
        share = jnp.exp(table_ref[pl.ds(at, groups), :] - total_ref[pl.ds(at, groups), :])
        wide = jnp.concatenate(
            [jnp.broadcast_to(share[g : g + 1, :], (D, D)) for g in range(groups)], axis=1
        )
        shift = xt_ref[:, pl.ds(start, CHUNK)] - jnp.concatenate([centre] * groups, axis=1)
        scaled = shift * wide
        for g in range(groups):
            first = first + scaled[:, g * D : (g + 1) * D]
        left = jnp.concatenate(split2(scaled), axis=0)
        right = jnp.concatenate(split2(x_ref[pl.ds(start, CHUNK), :] - mean), axis=1)
        acc[...] += dot(left, right)
        return first, count + share

    first, count = lax.fori_loop(
        0, NPTS // CHUNK, step, (jnp.zeros((D, D), F32), jnp.zeros((groups, D), F32))
    )
    weight_sum = jnp.sum(jnp.sum(count, axis=0, keepdims=True), axis=1, keepdims=True)
    first_row = jnp.sum(jnp.transpose(first), axis=0, keepdims=True)
    second = acc[:D, :D] + acc[:D, D:] + acc[D:, :D] + acc[D:, D:]
    return weight_sum, first_row, second


def inverse_factor(covariance, work):
    work[:, :D] = covariance
    work[:, D:] = eye()
    place = lax.broadcasted_iota(jnp.int32, (8, D), 0)
    for p in range(D // 8):
        left = work[8 * p : 8 * p + 8, :D]
        right = work[8 * p : 8 * p + 8, D:]
        columns = [
            jnp.broadcast_to(left[:, 8 * p + a : 8 * p + a + 1], (8, D)) for a in range(8)
        ]
        for a in range(8):
            pivot = jnp.broadcast_to(columns[a][a : a + 1, :], (8, D))
            scale = lax.rsqrt(pivot)
            scale = scale * (1.5 - 0.5 * pivot * scale * scale)
            column = columns[a] * scale
            below = jnp.where(place > a, column, 0.0)
            row_left = jnp.broadcast_to(left[a : a + 1, :], (8, D)) * scale
            row_right = jnp.broadcast_to(right[a : a + 1, :], (8, D)) * scale
            left = jnp.where(place == a, row_left, left - below * row_left)
            right = jnp.where(place == a, row_right, right - below * row_right)
            for b in range(a + 1, 8):
                columns[b] = columns[b] - below * jnp.broadcast_to(column[b : b + 1, :], (8, D))
        work[8 * p : 8 * p + 8, D:] = right
        if p + 1 < D // 8:
            h1, m1, l1 = [part.astype(F32) for part in split3(left)]
            both = jnp.concatenate([left, right], axis=1)
            h2, m2, l2 = [part.astype(F32) for part in split3(both)]
            one = jnp.concatenate([h1, h1, m1, h1, m1, l1], axis=0).astype(BF16)
            two = jnp.concatenate([h2, m2, h2, l2, m2, h2], axis=0).astype(BF16)
            change = lax.dot_general(
                one, two, (((0,), (0,)), ((), ())), preferred_element_type=F32
            )
            work[8 * p + 8 :, :] = work[8 * p + 8 :, :] - change[8 * p + 8 :, :]
    return work[:, D:]


def updated(x_ref, xt_ref, table_ref, total_ref, mean_ref, acc, work):
    mean = mean_ref[...]
    weight_sum, first, second = moments(x_ref, xt_ref, table_ref, total_ref, mean, acc)
    counted = weight_sum + 1.0
    covariance = (second - spread(first) * (first / counted) + eye()) / counted
    covariance = 0.5 * (covariance + jnp.transpose(covariance))
    lower_inverse = inverse_factor(covariance, work)
    new_mean = mean + first / counted
    new_weight = jnp.log(counted / float(NPTS + NZ * NY * NC * NX))
    return new_mean, jnp.transpose(lower_inverse), new_weight


def middle_kernel(
    x_ref, xt_ref, table_ref, total_ref, mean_ref, new_mean_ref, new_table_ref, acc, work
):
    mean, factor, weight = updated(x_ref, xt_ref, table_ref, total_ref, mean_ref, acc, work)
    new_mean_ref[...] = mean
    density(xt_ref, new_table_ref, mean, factor, weight)


def last_kernel(
    x_ref, xt_ref, table_ref, total_ref, mean_ref,
    new_mean_ref, new_factor_ref, new_weight_ref, acc, work,
):
    mean, factor, weight = updated(x_ref, xt_ref, table_ref, total_ref, mean_ref, acc, work)
    new_mean_ref[...] = mean
    new_factor_ref[...] = factor
    new_weight_ref[...] = jnp.broadcast_to(weight, (1, D))


def shape(*dims):
    return jax.ShapeDtypeStruct(dims, F32)


def local_call(kernel, outs, args, scratch, name):
    return pl.pallas_call(
        kernel,
        out_shape=outs,
        in_specs=[vmem()] * len(args),
        out_specs=[vmem()] * len(outs),
        scratch_shapes=scratch,
        compiler_params=pltpu.CompilerParams(vmem_limit_bytes=VMEM_LIMIT),
        name=name,
    )(*args)


SCRATCH = [pltpu.VMEM((2 * D, 2 * D), F32), pltpu.VMEM((D, 2 * D), F32)]


def first_density(x, mean, factor, weight):
    return local_call(
        first_density_kernel, [shape(D, NPTS), shape(ROWS, D)], (x, mean, factor, weight), [],
        "first_density",
    )


def middle(x, xt, table, total, mean):
    return local_call(
        middle_kernel, [shape(1, D), shape(ROWS, D)], (x, xt, table, total, mean), SCRATCH,
        "update_and_density",
    )


def last(x, xt, table, total, mean):
    return local_call(
        last_kernel, [shape(1, D), shape(D, D), shape(1, D)], (x, xt, table, total, mean),
        SCRATCH, "update",
    )


def own_densities(total, block_counts, block_dest):
    d = lax.axis_index(DP)
    prefix = jnp.cumsum(block_counts) - block_counts
    j = jnp.arange(block_dest.shape[1], dtype=jnp.int32)
    mine = ((block_dest == d) & (j[None, :] < block_counts[:, None])).reshape(-1)
    number = (prefix[:, None] + j[None, :]).reshape(-1)
    mine = mine.astype(jnp.int32)
    rank = jnp.cumsum(mine) - mine
    want = jnp.arange(RB, dtype=jnp.int32)
    p = jnp.sum(
        mine[None, :] * (rank[None, :] == want[:, None]).astype(jnp.int32) * number[None, :], axis=1
    )
    x = p % NX
    k = p // NX % NC
    y = p // (NX * NC) % NY
    z = p // (NX * NC * NY)
    flat = total.reshape(-1)
    a = flat[:BASE_B].reshape(-1, RA)[offset_a(k, x, y, z) // RA]
    b = flat[BASE_B:BASE_C].reshape(-1, RB_)[(offset_b(k, y, z, x) - BASE_B) // RB_]
    c = flat[BASE_C:].reshape(-1, RC)[(offset_c(k, z, x, y) - BASE_C) // RC]
    return jnp.concatenate([a, b, c], axis=1).reshape(-1)


def per_device(points, block_counts, block_dest, means, factors, log_weights):
    slots, from_slot, own_slot = live_slots(points, block_counts)
    x = gathered_points(slots, from_slot, own_slot)
    xt, table = first_density(x, means, factors[0], log_weights.reshape(1, 1))
    total = log_totals(table)
    mean, table = middle(x, xt, table, total, means)
    total = log_totals(table)
    new_mean, new_factor, new_weight = last(x, xt, table, total, mean)
    density_out = own_densities(total, block_counts, block_dest) / float(D)
    return new_mean, new_factor[None], new_weight[0, :1], density_out


def solution(mesh):
    split = Mesh(mesh.devices.reshape(NZ, NY, NC, NX), DP_COMP)
    in_specs = (P(DP, None), P(), P(), P(DP_COMP, None), P(DP_COMP, None, None), P(DP_COMP))
    out_specs = (P(DP_COMP, None), P(DP_COMP, None, None), P(DP_COMP), P(DP))
    return jax.shard_map(
        per_device, mesh=split, in_specs=in_specs, out_specs=out_specs, check_vma=False
    )
```

```python
import math

import jax
import jax.numpy as jnp
from jax import lax
from jax.experimental import pallas as pl
from jax.experimental.pallas import tpu as pltpu
from jax.sharding import Mesh
from jax.sharding import PartitionSpec as P

D = 128
BR = 64
RB = 4
ITERS = 2
Z, Y, C, X = "dp_0", "dp_1", "dp_2", "comp"
DP = (Z, Y, C)
DP_COMP = (Z, Y, C, X)
NZ, NY, NC, NX = 8, 4, 2, 4
NPTS = NZ * NY * NC * NX * BR
ROWS = NPTS // D
NB = 16
NSIDE = NY * NC
GROUP = NSIDE * NX
PIECE = ROWS // (NC * NX)
RA, RB_, RC = 24, 24, 16
BASE_B = NZ * NY * NC * NX * RA
BASE_C = BASE_B + NZ * NY * NC * NX * RB_
CHUNK = 2048
LOG_TWO_PI = math.log(2.0 * math.pi)
MESH = pl.DeviceIdType.MESH
F32, BF16 = jnp.float32, jnp.bfloat16
VMEM_LIMIT = 60 * 1024 * 1024


def vmem():
    return pl.BlockSpec(memory_space=pltpu.VMEM)


def smem():
    return pl.BlockSpec(memory_space=pltpu.SMEM)


def here():
    return lax.axis_index(Z), lax.axis_index(Y), lax.axis_index(C), lax.axis_index(X)


def shifted(place, step, size):
    return lax.rem(place + (step + size), size)


def split2(value):
    high = value.astype(BF16)
    return high, (value - high.astype(F32)).astype(BF16)


def split3(value):
    high = value.astype(BF16)
    rest = value - high.astype(F32)
    middle = rest.astype(BF16)
    return high, middle, (rest - middle.astype(F32)).astype(BF16)


def dot(a, b):
    return jnp.dot(a, b, preferred_element_type=F32)


def eye():
    return (
        lax.broadcasted_iota(jnp.int32, (D, D), 0) == lax.broadcasted_iota(jnp.int32, (D, D), 1)
    ).astype(F32)


def spread(row):
    return jnp.transpose(jnp.broadcast_to(row, (D, D)))


def moments(x_ref, xt_ref, table_ref, total_ref, mean, acc):
    centre = spread(mean)
    groups = CHUNK // D
    acc[...] = jnp.zeros_like(acc)

    def step(i, carry):
        first, count = carry
        start = pl.multiple_of(i * CHUNK, CHUNK)
        at = pl.multiple_of(i * groups, groups)
        share = jnp.exp(table_ref[pl.ds(at, groups), :] - total_ref[pl.ds(at, groups), :])
        wide = jnp.concatenate(
            [jnp.broadcast_to(share[g : g + 1, :], (D, D)) for g in range(groups)], axis=1
        )
        shift = xt_ref[:, pl.ds(start, CHUNK)] - jnp.concatenate([centre] * groups, axis=1)
        scaled = shift * wide
        for g in range(groups):
            first = first + scaled[:, g * D : (g + 1) * D]
        left = jnp.concatenate(split2(scaled), axis=0)
        right = jnp.concatenate(split2(x_ref[pl.ds(start, CHUNK), :] - mean), axis=1)
        acc[...] += dot(left, right)
        return first, count + share

    first, count = lax.fori_loop(
        0, NPTS // CHUNK, step, (jnp.zeros((D, D), F32), jnp.zeros((groups, D), F32))
    )
    weight_sum = jnp.sum(jnp.sum(count, axis=0, keepdims=True), axis=1, keepdims=True)
    first_row = jnp.sum(jnp.transpose(first), axis=0, keepdims=True)
    second = acc[:D, :D] + acc[:D, D:] + acc[D:, :D] + acc[D:, D:]
    return weight_sum, first_row, second


def inverse_factor(covariance, work):
    work[:, :D] = covariance
    work[:, D:] = eye()
    place = lax.broadcasted_iota(jnp.int32, (8, D), 0)
    last = D // 8

    def wide(row):
        return jnp.broadcast_to(row, (8, D))

    for p in range(last):
        at = 8 * p
        left, right = work[at : at + 8, :D], work[at : at + 8, D:]
        columns = [wide(left[:, at + a : at + a + 1]) for a in range(8)]
        if p + 1 < last:
            left1, right1 = work[at + 8 : at + 16, :D], work[at + 8 : at + 16, D:]
            columns1 = [wide(left1[:, at + a : at + a + 1]) for a in range(8)]
        for a in range(8):
            pivot = wide(columns[a][a : a + 1, :])
            scale = lax.rsqrt(pivot)
            column = columns[a] * scale
            below = jnp.where(place > a, column, 0.0)
            row_left = wide(left[a : a + 1, :]) * scale
            row_right = wide(right[a : a + 1, :]) * scale
            left = jnp.where(place == a, row_left, left - below * row_left)
            right = jnp.where(place == a, row_right, right - below * row_right)
            across = [wide(column[b : b + 1, :]) for b in range(a + 1, 8)]
            for b in range(a + 1, 8):
                columns[b] = columns[b] - below * across[b - a - 1]
            if p + 1 < last:
                below1 = columns1[a] * scale
                left1 = left1 - below1 * row_left
                right1 = right1 - below1 * row_right
                for b in range(a + 1, 8):
                    columns1[b] = columns1[b] - below1 * across[b - a - 1]
        work[at : at + 8, D:] = right
        if p + 1 < last:
            work[at + 8 : at + 16, :D] = left1
            work[at + 8 : at + 16, D:] = right1
        if p + 2 < last:
            h1, m1, l1 = [part.astype(F32) for part in split3(left)]
            both = jnp.concatenate([left, right], axis=1)
            h2, m2, l2 = [part.astype(F32) for part in split3(both)]
            one = jnp.concatenate([h1, h1, m1, h1, m1, l1], axis=0).astype(BF16)
            two = jnp.concatenate([h2, m2, h2, l2, m2, h2], axis=0).astype(BF16)
            change = lax.dot_general(
                one, two, (((0,), (0,)), ((), ())), preferred_element_type=F32
            )
            work[at + 16 :, :] = work[at + 16 :, :] - change[at + 16 :, :]
    return work[:, D:]


def offset_a(k, x, y=0, z=0):
    return (((k * NX + x) * NY + y) * NZ + z) * RA


def offset_b(k, y, z=0, x=0):
    return BASE_B + (((k * NY + y) * NZ + z) * NX + x) * RB_


def offset_c(k, z, x=0, y=0):
    return BASE_C + (((k * NZ + z) * NX + x) * NY + y) * RC


def remote(src, dst, ssem, rsem, target):
    return pltpu.make_async_remote_copy(
        src_ref=src, dst_ref=dst, send_sem=ssem, recv_sem=rsem,
        device_id=target, device_id_type=MESH,
    )


def side_at(side, step):
    t = shifted(side, step, NSIDE)
    return {Y: t // NC, C: lax.rem(t, NC)}


def enter(z, y, k, x):
    barrier = pltpu.get_barrier_semaphore()
    side = y * NC + k
    targets = [side_at(side, step) for step in range(1, NSIDE)]
    targets += [{Z: shifted(z, step, NZ)} for step in range(1, NZ)]
    targets += [{X: shifted(x, step, NX)} for step in range(1, NX)]
    for target in targets:
        pl.semaphore_signal(barrier, inc=1, device_id=target, device_id_type=MESH)
    return barrier, len(targets)


def choose_blocks(counts, prefix, z, y, k, x):
    mine = (y * NC + k) * NX + x
    own = z * GROUP + mine

    def step(s, carry):
        before, first = carry
        prefix[s] = before
        return before + counts[s], first + (before <= own).astype(jnp.int32)

    _, first = lax.fori_loop(0, NZ * NSIDE, step, (jnp.int32(0), jnp.int32(-1)))
    start = prefix[z * NSIDE + y * NC + k]
    blocks = [
        jnp.minimum(jnp.bitwise_and(t * NX + x - start, GROUP - 1), NB - 1) for t in range(NSIDE)
    ]
    from_slot = [jnp.int32(0)] * NZ
    for t in range(NSIDE):
        sender = z * NSIDE + t
        j = jnp.bitwise_and(mine - prefix[sender], GROUP - 1)
        to_z = jnp.where(j < counts[sender], (prefix[sender] + j) // GROUP, NZ)
        from_slot = [jnp.where(to_z == i, t, from_slot[i]) for i in range(NZ)]
    return blocks, from_slot, first // NSIDE


def log_totals(table, out, r0, v, rx, u, ry, w, rz, sem, z, y, k, x):
    other = {C: 1 - k}
    number = [0]

    def copy_to(src, dst, target):
        n = number[0]
        number[0] += 1
        copy = remote(src, dst, sem.at[0, n], sem.at[1, n], target)
        copy.start()
        return copy

    def joined(parts):
        peak = parts[0]
        for part in parts[1:]:
            peak = jnp.maximum(peak, part)
        total = jnp.exp(parts[0] - peak)
        for part in parts[1:]:
            total = total + jnp.exp(part - peak)
        return peak + jnp.log(total)

    half = ROWS // NC
    copy_to(table.at[pl.ds(pl.multiple_of((1 - k) * half, 8), half)], r0, other).wait()
    v[...] = joined([table[pl.ds(pl.multiple_of(k * half, 8), half), :], r0[...]])

    def piece(at):
        return pl.ds(pl.multiple_of(at * PIECE, 8), PIECE)

    copies = [
        copy_to(v.at[piece(shifted(x, step, NX))], rx.at[step - 1], {X: shifted(x, step, NX)})
        for step in range(1, NX)
    ]
    for copy in copies:
        copy.wait()
    u[...] = joined([v[piece(x), :]] + [rx[i] for i in range(NX - 1)])
    copies = [
        copy_to(u, ry.at[step - 1], {Y: shifted(y, step, NY)}) for step in range(1, NY)
    ]
    for copy in copies:
        copy.wait()
    w[...] = joined([u[...]] + [ry[i] for i in range(NY - 1)])
    copies = [
        copy_to(w, rz.at[step - 1], {Z: shifted(z, step, NZ)}) for step in range(1, NZ)
    ]
    for copy in copies:
        copy.wait()
    mine = piece(k * NX + x)
    out[mine, :] = joined([w[...]] + [rz[i] for i in range(NZ - 1)])
    part = out.at[mine]
    copies = [copy_to(part, part, {X: shifted(x, step, NX)}) for step in range(1, NX)]
    to_other = [copy_to(part, part, other)]
    for step in range(1, NX):
        copies[step - 1].wait()
        part = out.at[piece(k * NX + shifted(x, -step, NX))]
        to_other.append(copy_to(part, part, other))
    for copy in to_other:
        copy.wait()


N_LSE = 1 + 3 * (NX - 1) + 1 + (NY - 1) + (NZ - 1)


def prepare(mean, factor, weight, main, rest, centre, offset):
    high, middle, low = split3(jnp.transpose(factor))
    main[:D, :D] = high
    main[:D, D:] = high
    main[D:, :D] = middle
    main[D:, D:] = middle
    rest[:, :D] = high
    rest[:, D:] = low
    centre[...] = spread(mean)
    diagonal = jnp.sum(factor * eye(), axis=0, keepdims=True)
    offset[...] = jnp.broadcast_to(
        weight + jnp.sum(jnp.log(diagonal), axis=1, keepdims=True) - 0.5 * D * LOG_TWO_PI, (1, D)
    )


def density(turned, table, first_group, main, rest, centre, offset):
    groups = turned.shape[1] // D
    shift = turned - jnp.concatenate([centre[...]] * groups, axis=1)
    a, b, c = split3(shift)
    both = dot(main[...], jnp.concatenate([a, b], axis=0))
    value = both[:D] + both[D:] + dot(rest[...], jnp.concatenate([c, a], axis=0))
    total = jnp.sum(value * value, axis=0, keepdims=True)
    for g in range(groups):
        table[pl.ds(first_group + g, 1), :] = offset[...] - 0.5 * total[:, g * D : (g + 1) * D]


def updated(x_ref, xt_ref, table_ref, total_ref, mean, acc, work):
    weight_sum, first, second = moments(x_ref, xt_ref, table_ref, total_ref, mean, acc)
    counted = weight_sum + 1.0
    covariance = (second - spread(first) * (first / counted) + eye()) / counted
    covariance = 0.5 * (covariance + jnp.transpose(covariance))
    lower_inverse = inverse_factor(covariance, work)
    new_mean = mean + first / counted
    new_weight = jnp.log(counted / float(NPTS + NZ * NY * NC * NX))
    return new_mean, jnp.transpose(lower_inverse), new_weight


def step_kernel(
    counts, points, mean_ref, factor_ref, weight_ref,
    new_mean_ref, new_factor_ref, new_weight_ref, total_ref,
    prefix, slots, r1, s2, r2, out, xt, table1, table2, total1, mean2,
    main, rest, centre, offset, acc, work, sem1, sem2, semg, sems, semk, *joins,
):
    z, y, k, x = here()
    side = y * NC + k
    barrier, arrivals = enter(z, y, k, x)
    blocks, from_slot, own_slot = choose_blocks(counts, prefix, z, y, k, x)
    for t in range(NSIDE):
        slots[t] = points[blocks[t]]
    pl.semaphore_wait(barrier, arrivals)

    copies = []
    for step in range(1, NSIDE):
        copies.append(
            remote(
                slots.at[shifted(side, step, NSIDE)], r1.at[side],
                sem1.at[0, step], sem1.at[1, step], side_at(side, step),
            )
        )
        copies[-1].start()
    r1[side] = slots[side]
    prepare(mean_ref[...], factor_ref[...], weight_ref[...], main, rest, centre, offset)
    for copy in copies:
        copy.wait()
    for t in range(NZ):
        s2[t] = r1[from_slot[t]]
    copies = []
    for step in range(1, NZ):
        t = shifted(z, step, NZ)
        copies.append(remote(s2.at[t], r2.at[z], sem2.at[0, step], sem2.at[1, step], {Z: t}))
        copies[-1].start()
    r2[z] = s2[z]
    for copy in copies:
        copy.wait()
    block = r2[own_slot]

    def rows(start, size):
        return out.at[pl.ds(pl.multiple_of(start, 8), size)]

    rows(offset_a(k, x, y, z), RA)[...] = block[:RA]
    rows(offset_b(k, y, z, x), RB_)[...] = block[RA : RA + RB_]
    rows(offset_c(k, z, x, y), RC)[...] = block[RA + RB_ :]

    number = [0]

    def spread_out(axis, place, size, start, count):
        part = rows(start, count)
        copies = []
        for step in range(1, size):
            n = number[0]
            number[0] += 1
            copies.append(
                remote(
                    part, part, semg.at[0, n], semg.at[1, n], {axis: shifted(place, step, size)}
                )
            )
            copies[-1].start()
        return copies

    def finish(copies):
        for copy in copies:
            copy.wait()

    first_b = spread_out(X, x, NX, offset_b(k, y, z, x), RB_)
    first_c = spread_out(Y, y, NY, offset_c(k, z, x, y), RC)
    first_a = spread_out(Z, z, NZ, offset_a(k, x, y, z), RA)
    finish(first_b)
    second_b = spread_out(Z, z, NZ, offset_b(k, y, z), NX * RB_)
    finish(first_c)
    second_c = spread_out(X, x, NX, offset_c(k, z, x), NY * RC)
    finish(first_a)
    second_a = spread_out(Y, y, NY, offset_a(k, x, y), NZ * RA)

    other = {C: 1 - k}
    rings = (
        (X, x, NX, offset_a, NY * NZ * RA),
        (Y, y, NY, offset_b, NZ * NX * RB_),
        (Z, z, NZ, offset_c, NX * NY * RC),
    )
    pieces = {}
    waiting = []
    to_other = []
    theirs = []

    def start_of(ring, core, at, half):
        return rings[ring][3](core, at) + half * (rings[ring][4] // 2)

    def pass_on(ring, at, half, size):
        part = rows(start_of(ring, k, at, half), size)
        n = len(to_other)
        to_other.append(remote(part, part, semk.at[0, n], semk.at[1, n], other))
        to_other[-1].start()
        theirs.append((start_of(ring, 1 - k, at, half), size))

    def work_out(start, size):
        unit = min(size, 3 * D)
        for i in range(0, size, unit):
            at = pl.multiple_of(start + i, D)
            turned = jnp.transpose(out[pl.ds(at, unit), :])
            xt[:, pl.ds(at, unit)] = turned
            density(turned, table1, at // D, main, rest, centre, offset)

    def send(ring, way, step, half):
        axis, place, size, _, unit = rings[ring]
        at = shifted(place, -way * (step - 1), size)
        part = rows(start_of(ring, k, at, half), unit // 2)
        n = len(waiting)
        copy = remote(
            part, part, sems.at[0, n], sems.at[1, n], {axis: shifted(place, way, size)}
        )
        copy.start()
        waiting.append(copy)
        pieces[ring, way, step, half] = copy

    order = []
    for ring in (0, 1, 2):
        steps = rings[ring][2] // 2
        begin, scale = (16.3, 4.2) if ring < 2 else (11.5, 1.5)
        for step in range(1, steps + 1):
            for late in (0, 1):
                if step == steps and late:
                    continue
                for way in (1, -1):
                    half = late if way == 1 else 1 - late
                    order.append((begin + scale * (2 * step + late - 1), ring, way, step, half))
    order.sort(key=lambda row: row[0])

    def begin_ring(ring):
        for _, other_ring, way, step, half in order:
            if other_ring == ring and step == 1:
                send(ring, way, step, half)
        pass_on(ring, rings[ring][1], 0, rings[ring][4])

    finish(second_c)
    begin_ring(2)
    work_out(start_of(2, k, z, 0), rings[2][4])
    finish(second_a)
    begin_ring(0)
    finish(second_b)
    begin_ring(1)
    work_out(start_of(0, k, x, 0), rings[0][4])
    work_out(start_of(1, k, y, 0), rings[1][4])
    done = 0
    for _, ring, way, step, half in order:
        axis, place, size, _, unit = rings[ring]
        pieces[ring, way, step, half].wait_recv()
        steps = size // 2
        if step + 1 < steps or (step + 1 == steps and half == (0 if way == 1 else 1)):
            send(ring, way, step + 1, half)
        at = shifted(place, -way * step, size)
        pass_on(ring, at, half, unit // 2)
        work_out(start_of(ring, k, at, half), unit // 2)
        to_other[done].wait_recv()
        work_out(*theirs[done])
        done += 1
    while done < len(to_other):
        to_other[done].wait_recv()
        work_out(*theirs[done])
        done += 1
    for copy in waiting + to_other:
        copy.wait_send()

    half = len(joins) // ITERS
    log_totals(table1, total1, *joins[:half], z, y, k, x)
    mean, factor, weight = updated(out, xt, table1, total1, mean_ref[...], acc, work)
    mean2[...] = mean
    prepare(mean, factor, weight, main, rest, centre, offset)

    def again(i, carry):
        start = pl.multiple_of(i * CHUNK, CHUNK)
        density(
            xt[:, pl.ds(start, CHUNK)], table2, i * (CHUNK // D), main, rest, centre, offset
        )
        return carry

    lax.fori_loop(0, NPTS // CHUNK, again, 0)
    log_totals(table2, total_ref, *joins[half:], z, y, k, x)
    mean, factor, weight = updated(out, xt, table2, total_ref, mean2[...], acc, work)
    new_mean_ref[...] = mean
    new_factor_ref[...] = factor
    new_weight_ref[...] = jnp.broadcast_to(weight, (1, D))


N_DIRECT = 2 * (NZ - 1) + 2 * (NX - 1) + 2 * (NY - 1)
N_RING = 2 * (NX - 1) + 2 * (NY - 1) + 2 * (NZ - 1)
N_OTHER = N_RING + 3


def shape(*dims):
    return jax.ShapeDtypeStruct(dims, F32)


def join_scratch():
    return [
        pltpu.VMEM((ROWS // NC, D), F32),
        pltpu.VMEM((ROWS // NC, D), F32),
        pltpu.VMEM((NX - 1, PIECE, D), F32),
        pltpu.VMEM((PIECE, D), F32),
        pltpu.VMEM((NY - 1, PIECE, D), F32),
        pltpu.VMEM((PIECE, D), F32),
        pltpu.VMEM((NZ - 1, PIECE, D), F32),
        pltpu.SemaphoreType.DMA((2, N_LSE)),
    ]


def whole_step(counts, points, mean, factor, weight):
    sem = pltpu.SemaphoreType.DMA
    return pl.pallas_call(
        step_kernel,
        out_shape=[shape(1, D), shape(D, D), shape(1, D), shape(ROWS, D)],
        in_specs=[smem()] + [vmem()] * 4,
        out_specs=[vmem()] * 4,
        scratch_shapes=[
            pltpu.SMEM((NZ * NSIDE,), jnp.int32),
            pltpu.VMEM((NSIDE, BR, D), F32),
            pltpu.VMEM((NSIDE, BR, D), F32),
            pltpu.VMEM((NZ, BR, D), F32),
            pltpu.VMEM((NZ, BR, D), F32),
            pltpu.VMEM((NPTS, D), F32),
            pltpu.VMEM((D, NPTS), F32),
            pltpu.VMEM((ROWS, D), F32),
            pltpu.VMEM((ROWS, D), F32),
            pltpu.VMEM((ROWS, D), F32),
            pltpu.VMEM((1, D), F32),
            pltpu.VMEM((2 * D, 2 * D), BF16),
            pltpu.VMEM((D, 2 * D), BF16),
            pltpu.VMEM((D, D), F32),
            pltpu.VMEM((1, D), F32),
            pltpu.VMEM((2 * D, 2 * D), F32),
            pltpu.VMEM((D, 2 * D), F32),
            sem((2, NSIDE)), sem((2, NZ)), sem((2, N_DIRECT)), sem((2, N_RING)),
            sem((2, N_OTHER)),
        ]
        + join_scratch() * ITERS,
        compiler_params=pltpu.CompilerParams(
            collective_id=0, has_side_effects=True, vmem_limit_bytes=VMEM_LIMIT
        ),
        name="whole_step",
    )(counts, points, mean, factor, weight)


def own_densities(total, block_counts, block_dest):
    d = lax.axis_index(DP)
    prefix = jnp.cumsum(block_counts) - block_counts
    j = jnp.arange(block_dest.shape[1], dtype=jnp.int32)
    mine = ((block_dest == d) & (j[None, :] < block_counts[:, None])).reshape(-1)
    number = (prefix[:, None] + j[None, :]).reshape(-1)
    mine = mine.astype(jnp.int32)
    rank = jnp.cumsum(mine) - mine
    want = jnp.arange(RB, dtype=jnp.int32)
    p = jnp.sum(
        mine[None, :] * (rank[None, :] == want[:, None]).astype(jnp.int32) * number[None, :], axis=1
    )
    x = p % NX
    k = p // NX % NC
    y = p // (NX * NC) % NY
    z = p // (NX * NC * NY)
    flat = total.reshape(-1)
    a = flat[:BASE_B].reshape(-1, RA)[offset_a(k, x, y, z) // RA]
    b = flat[BASE_B:BASE_C].reshape(-1, RB_)[(offset_b(k, y, z, x) - BASE_B) // RB_]
    c = flat[BASE_C:].reshape(-1, RC)[(offset_c(k, z, x, y) - BASE_C) // RC]
    return jnp.concatenate([a, b, c], axis=1).reshape(-1)


def per_device(points, block_counts, block_dest, means, factors, log_weights):
    new_mean, new_factor, new_weight, total = whole_step(
        block_counts, points.reshape(NB, BR, D), means, factors[0], log_weights.reshape(1, 1)
    )
    density_out = own_densities(total, block_counts, block_dest) / float(D)
    return new_mean, new_factor[None], new_weight[0, :1], density_out


def solution(mesh):
    split = Mesh(mesh.devices.reshape(NZ, NY, NC, NX), DP_COMP)
    in_specs = (P(DP, None), P(), P(), P(DP_COMP, None), P(DP_COMP, None, None), P(DP_COMP))
    out_specs = (P(DP_COMP, None), P(DP_COMP, None, None), P(DP_COMP), P(DP))
    return jax.shard_map(
        per_device, mesh=split, in_specs=in_specs, out_specs=out_specs, check_vma=False
    )
```

```python
import math

import jax
import jax.numpy as jnp
from jax import lax
from jax.experimental import pallas as pl
from jax.experimental.pallas import tpu as pltpu
from jax.sharding import Mesh
from jax.sharding import PartitionSpec as P

D = 128
BR = 64
RB = 4
ITERS = 2
Z, Y, C, X = "dp_0", "dp_1", "dp_2", "comp"
DP = (Z, Y, C)
DP_COMP = (Z, Y, C, X)
NZ, NY, NC, NX = 8, 4, 2, 4
NPTS = NZ * NY * NC * NX * BR
ROWS = NPTS // D
NB = 16
NSIDE = NY * NC
GROUP = NSIDE * NX
PARTS = 2
PIECE = ROWS // (PARTS * NC * NX)
RA, RB_, RC = 24, 24, 16
BASE_B = NZ * NY * NC * NX * RA
BASE_C = BASE_B + NZ * NY * NC * NX * RB_
CHUNK = 2048
LOG_TWO_PI = math.log(2.0 * math.pi)
MESH = pl.DeviceIdType.MESH
F32, BF16 = jnp.float32, jnp.bfloat16
VMEM_LIMIT = 60 * 1024 * 1024


def vmem():
    return pl.BlockSpec(memory_space=pltpu.VMEM)


def smem():
    return pl.BlockSpec(memory_space=pltpu.SMEM)


def here():
    return lax.axis_index(Z), lax.axis_index(Y), lax.axis_index(C), lax.axis_index(X)


def shifted(place, step, size):
    return lax.rem(place + (step + size), size)


def split2(value):
    high = value.astype(BF16)
    return high, (value - high.astype(F32)).astype(BF16)


def split3(value):
    high = value.astype(BF16)
    rest = value - high.astype(F32)
    middle = rest.astype(BF16)
    return high, middle, (rest - middle.astype(F32)).astype(BF16)


def dot(a, b):
    return jnp.dot(a, b, preferred_element_type=F32)


def eye():
    return (
        lax.broadcasted_iota(jnp.int32, (D, D), 0) == lax.broadcasted_iota(jnp.int32, (D, D), 1)
    ).astype(F32)


def spread(row):
    return jnp.transpose(jnp.broadcast_to(row, (D, D)))


def moments(x_ref, xt_ref, table_ref, base, total_ref, mean, acc, part, carry):
    centre = spread(mean)
    groups = CHUNK // D
    steps = NPTS // CHUNK // PARTS

    def step(i, carry):
        first, count = carry
        start = pl.multiple_of(i * CHUNK, CHUNK)
        at = pl.multiple_of((i - part * steps) * groups, groups)
        share = jnp.exp(table_ref[pl.ds(base + at, groups), :] - total_ref[pl.ds(at, groups), :])
        wide = jnp.concatenate(
            [jnp.broadcast_to(share[g : g + 1, :], (D, D)) for g in range(groups)], axis=1
        )
        shift = xt_ref[:, pl.ds(start, CHUNK)] - jnp.concatenate([centre] * groups, axis=1)
        scaled = shift * wide
        for g in range(groups):
            first = first + scaled[:, g * D : (g + 1) * D]
        left = jnp.concatenate(split2(scaled), axis=0)
        right = jnp.concatenate(split2(x_ref[pl.ds(start, CHUNK), :] - mean), axis=1)
        acc[...] += dot(left, right)
        return first, count + share

    if part == 0:
        acc[...] = jnp.zeros_like(acc)
        carry = (jnp.zeros((D, D), F32), jnp.zeros((groups, D), F32))
    return lax.fori_loop(part * steps, (part + 1) * steps, step, carry)


def moment_sums(acc, carry):
    first, count = carry
    weight_sum = jnp.sum(jnp.sum(count, axis=0, keepdims=True), axis=1, keepdims=True)
    first_row = jnp.sum(jnp.transpose(first), axis=0, keepdims=True)
    second = acc[:D, :D] + acc[:D, D:] + acc[D:, :D] + acc[D:, D:]
    return weight_sum, first_row, second


def inverse_factor(covariance, work):
    work[:, :D] = covariance
    work[:, D:] = eye()
    place = lax.broadcasted_iota(jnp.int32, (8, D), 0)
    last = D // 8

    def wide(row):
        return jnp.broadcast_to(row, (8, D))

    for p in range(last):
        at = 8 * p
        left, right = work[at : at + 8, :D], work[at : at + 8, D:]
        columns = [wide(left[:, at + a : at + a + 1]) for a in range(8)]
        if p + 1 < last:
            left1, right1 = work[at + 8 : at + 16, :D], work[at + 8 : at + 16, D:]
            columns1 = [wide(left1[:, at + a : at + a + 1]) for a in range(8)]
        for a in range(8):
            pivot = wide(columns[a][a : a + 1, :])
            scale = lax.rsqrt(pivot)
            column = columns[a] * scale
            below = jnp.where(place > a, column, 0.0)
            row_left = wide(left[a : a + 1, :]) * scale
            row_right = wide(right[a : a + 1, :]) * scale
            left = jnp.where(place == a, row_left, left - below * row_left)
            right = jnp.where(place == a, row_right, right - below * row_right)
            across = [wide(column[b : b + 1, :]) for b in range(a + 1, 8)]
            for b in range(a + 1, 8):
                columns[b] = columns[b] - below * across[b - a - 1]
            if p + 1 < last:
                below1 = columns1[a] * scale
                left1 = left1 - below1 * row_left
                right1 = right1 - below1 * row_right
                for b in range(a + 1, 8):
                    columns1[b] = columns1[b] - below1 * across[b - a - 1]
        work[at : at + 8, D:] = right
        if p + 1 < last:
            work[at + 8 : at + 16, :D] = left1
            work[at + 8 : at + 16, D:] = right1
        if p + 2 < last:
            h1, m1, l1 = [part.astype(F32) for part in split3(left)]
            both = jnp.concatenate([left, right], axis=1)
            h2, m2, l2 = [part.astype(F32) for part in split3(both)]
            one = jnp.concatenate([h1, h1, m1, h1, m1, l1], axis=0).astype(BF16)
            two = jnp.concatenate([h2, m2, h2, l2, m2, h2], axis=0).astype(BF16)
            change = lax.dot_general(
                one, two, (((0,), (0,)), ((), ())), preferred_element_type=F32
            )
            work[at + 16 :, :] = work[at + 16 :, :] - change[at + 16 :, :]
    return work[:, D:]


def offset_a(k, x, y=0, z=0):
    return (((k * NX + x) * NY + y) * NZ + z) * RA


def offset_b(k, y, z=0, x=0):
    return BASE_B + (((k * NY + y) * NZ + z) * NX + x) * RB_


def offset_c(k, z, x=0, y=0):
    return BASE_C + (((k * NZ + z) * NX + x) * NY + y) * RC


def remote(src, dst, ssem, rsem, target):
    return pltpu.make_async_remote_copy(
        src_ref=src, dst_ref=dst, send_sem=ssem, recv_sem=rsem,
        device_id=target, device_id_type=MESH,
    )


def side_at(side, step):
    t = shifted(side, step, NSIDE)
    return {Y: t // NC, C: lax.rem(t, NC)}


def enter(z, y, k, x):
    barrier = pltpu.get_barrier_semaphore()
    side = y * NC + k
    targets = [side_at(side, step) for step in range(1, NSIDE)]
    targets += [{Z: shifted(z, step, NZ)} for step in range(1, NZ)]
    targets += [{X: shifted(x, step, NX)} for step in range(1, NX)]
    targets += [{X: shifted(x, step, NX), C: 1 - k} for step in range(1, NX)]
    for target in targets:
        pl.semaphore_signal(barrier, inc=1, device_id=target, device_id_type=MESH)
    return barrier, len(targets)


def choose_blocks(counts, prefix, z, y, k, x):
    mine = (y * NC + k) * NX + x
    own = z * GROUP + mine

    def step(s, carry):
        before, first = carry
        prefix[s] = before
        return before + counts[s], first + (before <= own).astype(jnp.int32)

    _, first = lax.fori_loop(0, NZ * NSIDE, step, (jnp.int32(0), jnp.int32(-1)))
    start = prefix[z * NSIDE + y * NC + k]
    blocks = [
        jnp.minimum(jnp.bitwise_and(t * NX + x - start, GROUP - 1), NB - 1) for t in range(NSIDE)
    ]
    from_slot = [jnp.int32(0)] * NZ
    for t in range(NSIDE):
        sender = z * NSIDE + t
        j = jnp.bitwise_and(mine - prefix[sender], GROUP - 1)
        to_z = jnp.where(j < counts[sender], (prefix[sender] + j) // GROUP, NZ)
        from_slot = [jnp.where(to_z == i, t, from_slot[i]) for i in range(NZ)]
    return blocks, from_slot, first // NSIDE


def own_blocks(dests, counts, prefix, d):
    def step(s, carry):
        n, found = carry[0], carry[1:]
        at = jnp.int32(-1)
        for j in range(NB):
            at = jnp.where((dests[j, s] == d) & (j < counts[s]), j, at)
        number = prefix[s] + at
        here_too = at >= 0
        found = [jnp.where(here_too & (n == i), number, found[i]) for i in range(RB)]
        return (n + here_too.astype(jnp.int32), *found)

    return lax.fori_loop(0, NZ * NSIDE, step, (jnp.int32(0),) * (RB + 1))[1:]


def own_density(total, found, density_ref):
    lane = lax.broadcasted_iota(jnp.int32, (1, D), 1)
    line = jnp.zeros((1, D), F32)
    for i in range(RB):
        p = found[i]
        x = lax.rem(p, NX)
        k = lax.rem(lax.div(p, NX), NC)
        y = lax.rem(lax.div(p, NX * NC), NY)
        z = lax.div(p, GROUP)
        parts = (
            (0, offset_a(k, x, y, z), RA),
            (RA, offset_b(k, y, z, x), RB_),
            (RA + RB_, offset_c(k, z, x, y), RC),
        )
        for base, start, count in parts:
            row = lax.div(start, D)
            first = start - row * D
            to = (i % 2) * BR + base
            by = lax.rem(to - first + D, D)
            one = pltpu.roll(total[pl.ds(row, 1), :], by, 1)
            two = pltpu.roll(total[pl.ds(jnp.minimum(row + 1, ROWS - 1), 1), :], by, 1)
            value = jnp.where(lane - to + first < D, one, two)
            line = jnp.where((lane >= to) & (lane < to + count), value, line)
        if i % 2:
            density_ref[i // 2 : i // 2 + 1, :] = line / float(D)


def group_at(k, x, step):
    t = shifted(k * NX + x, step, NC * NX)
    return t, {C: t // NX, X: lax.rem(t, NX)}


def joined(parts):
    peak = parts[0]
    for part in parts[1:]:
        peak = jnp.maximum(peak, part)
    total = jnp.exp(parts[0] - peak)
    for part in parts[1:]:
        total = total + jnp.exp(part - peak)
    return peak + jnp.log(total)


def log_totals(table, base, out, rg, u, ry, w, rz, sem, z, y, k, x):
    members = NC * NX
    number = [0]

    def copy_to(src, dst, target):
        n = number[0]
        number[0] += 1
        copy = remote(src, dst, sem.at[0, n], sem.at[1, n], target)
        copy.start()
        return copy

    def piece(start, at):
        return pl.ds(pl.multiple_of(start + at * PIECE, 8), PIECE)

    mine = piece(0, k * NX + x)
    copies = []
    for step in range(1, members):
        at, target = group_at(k, x, step)
        copies.append(copy_to(table.at[piece(base, at)], rg.at[step - 1], target))
    yield
    for copy in copies:
        copy.wait()
    u[...] = joined([table[piece(base, k * NX + x), :]] + [rg[i] for i in range(members - 1)])
    copies = [
        copy_to(u, ry.at[step - 1], {Y: shifted(y, step, NY)}) for step in range(1, NY)
    ]
    yield
    for copy in copies:
        copy.wait()
    w[...] = joined([u[...]] + [ry[i] for i in range(NY - 1)])
    copies = [
        copy_to(w, rz.at[step - 1], {Z: shifted(z, step, NZ)}) for step in range(1, NZ)
    ]
    yield
    for copy in copies:
        copy.wait()
    out[mine, :] = joined([w[...]] + [rz[i] for i in range(NZ - 1)])
    copies = []
    for step in range(1, members):
        copies.append(copy_to(out.at[mine], out.at[mine], group_at(k, x, step)[1]))
    yield
    for copy in copies:
        copy.wait()


N_LSE = 2 * (NC * NX - 1) + (NY - 1) + (NZ - 1)


def prepare(mean, factor, weight, main, rest, centre, offset):
    high, middle, low = split3(jnp.transpose(factor))
    main[:D, :D] = high
    main[:D, D:] = high
    main[D:, :D] = middle
    main[D:, D:] = middle
    rest[:, :D] = high
    rest[:, D:] = low
    centre[...] = spread(mean)
    diagonal = jnp.sum(factor * eye(), axis=0, keepdims=True)
    offset[...] = jnp.broadcast_to(
        weight + jnp.sum(jnp.log(diagonal), axis=1, keepdims=True) - 0.5 * D * LOG_TWO_PI, (1, D)
    )


def density(turned, table, first_group, main, rest, centre, offset):
    groups = turned.shape[1] // D
    shift = turned - jnp.concatenate([centre[...]] * groups, axis=1)
    a, b, c = split3(shift)
    both = dot(main[...], jnp.concatenate([a, b], axis=0))
    value = both[:D] + both[D:] + dot(rest[...], jnp.concatenate([c, a], axis=0))
    total = jnp.sum(value * value, axis=0, keepdims=True)
    for g in range(groups):
        table[pl.ds(first_group + g, 1), :] = offset[...] - 0.5 * total[:, g * D : (g + 1) * D]


def updated(mean, acc, carry, work):
    weight_sum, first, second = moment_sums(acc, carry)
    counted = weight_sum + 1.0
    covariance = (second - spread(first) * (first / counted) + eye()) / counted
    covariance = 0.5 * (covariance + jnp.transpose(covariance))
    lower_inverse = inverse_factor(covariance, work)
    new_mean = mean + first / counted
    new_weight = jnp.log(counted / float(NPTS + NZ * NY * NC * NX))
    return new_mean, jnp.transpose(lower_inverse), new_weight


def step_kernel(
    counts, dests, points_ref, mean_ref, factor_ref, weight_ref,
    new_mean_ref, new_factor_ref, new_weight_ref, density_ref,
    prefix, points, slots, r1, s2, r2, out, xt, table1, table2a, table2b,
    total1a, total1b, total2a, total2b, total2, mean2,
    main, rest, centre, offset, acc, work, sem0, sem1, sem2, semg, sems, semk, *joins,
):
    z, y, k, x = here()
    side = y * NC + k
    load = pltpu.make_async_copy(points_ref, points, sem0)
    load.start()
    barrier, arrivals = enter(z, y, k, x)
    blocks, from_slot, own_slot = choose_blocks(counts, prefix, z, y, k, x)
    load.wait()
    for t in range(NSIDE):
        slots[t] = points[blocks[t]]
    pl.semaphore_wait(barrier, arrivals)

    copies = []
    for step in range(1, NSIDE):
        copies.append(
            remote(
                slots.at[shifted(side, step, NSIDE)], r1.at[side],
                sem1.at[0, step], sem1.at[1, step], side_at(side, step),
            )
        )
        copies[-1].start()
    r1[side] = slots[side]
    prepare(mean_ref[...], factor_ref[...], weight_ref[...], main, rest, centre, offset)
    for copy in copies:
        copy.wait()
    for t in range(NZ):
        s2[t] = r1[from_slot[t]]
    copies = []
    for step in range(1, NZ):
        t = shifted(z, step, NZ)
        copies.append(remote(s2.at[t], r2.at[z], sem2.at[0, step], sem2.at[1, step], {Z: t}))
        copies[-1].start()
    r2[z] = s2[z]
    found = own_blocks(dests, counts, prefix, z * NSIDE + side)
    for copy in copies:
        copy.wait()
    block = r2[own_slot]

    def rows(start, size):
        return out.at[pl.ds(pl.multiple_of(start, 8), size)]

    rows(offset_a(k, x, y, z), RA)[...] = block[:RA]
    rows(offset_b(k, y, z, x), RB_)[...] = block[RA : RA + RB_]
    rows(offset_c(k, z, x, y), RC)[...] = block[RA + RB_ :]

    number = [0]

    def spread_out(axis, place, size, start, count):
        part = rows(start, count)
        copies = []
        for step in range(1, size):
            n = number[0]
            number[0] += 1
            copies.append(
                remote(
                    part, part, semg.at[0, n], semg.at[1, n], {axis: shifted(place, step, size)}
                )
            )
            copies[-1].start()
        return copies

    def finish(copies):
        for copy in copies:
            copy.wait()

    first_b = spread_out(X, x, NX, offset_b(k, y, z, x), RB_)
    first_c = spread_out(Y, y, NY, offset_c(k, z, x, y), RC)
    first_a = spread_out(Z, z, NZ, offset_a(k, x, y, z), RA)
    finish(first_b)
    second_b = spread_out(Z, z, NZ, offset_b(k, y, z), NX * RB_)
    finish(first_c)
    second_c = spread_out(X, x, NX, offset_c(k, z, x), NY * RC)
    finish(first_a)
    second_a = spread_out(Y, y, NY, offset_a(k, x, y), NZ * RA)

    other = {C: 1 - k}
    rings = (
        (X, x, NX, offset_a, NY * NZ * RA),
        (Y, y, NY, offset_b, NZ * NX * RB_),
        (Z, z, NZ, offset_c, NX * NY * RC),
    )
    pieces = {}
    waiting = []
    to_other = []
    theirs = []

    def start_of(ring, core, at, half):
        return rings[ring][3](core, at) + half * (rings[ring][4] // 2)

    def pass_on(ring, at, half, size):
        part = rows(start_of(ring, k, at, half), size)
        n = len(to_other)
        to_other.append(remote(part, part, semk.at[0, n], semk.at[1, n], other))
        to_other[-1].start()
        theirs.append((start_of(ring, 1 - k, at, half), size))

    def work_out(start, size):
        unit = min(size, 3 * D)
        for i in range(0, size, unit):
            at = pl.multiple_of(start + i, D)
            turned = jnp.transpose(out[pl.ds(at, unit), :])
            xt[:, pl.ds(at, unit)] = turned
            density(turned, table1, at // D, main, rest, centre, offset)

    def send(ring, way, step, half):
        axis, place, size, _, unit = rings[ring]
        at = shifted(place, -way * (step - 1), size)
        part = rows(start_of(ring, k, at, half), unit // 2)
        n = len(waiting)
        copy = remote(
            part, part, sems.at[0, n], sems.at[1, n], {axis: shifted(place, way, size)}
        )
        copy.start()
        waiting.append(copy)
        pieces[ring, way, step, half] = copy

    order = []
    for ring in (0, 1, 2):
        steps = rings[ring][2] // 2
        begin, scale = (16.3, 4.2) if ring < 2 else (11.5, 1.5)
        for step in range(1, steps + 1):
            for late in (0, 1):
                if step == steps and late:
                    continue
                for way in (1, -1):
                    half = late if way == 1 else 1 - late
                    order.append((begin + scale * (2 * step + late - 1), ring, way, step, half))
    order.sort(key=lambda row: row[0])

    def begin_ring(ring):
        for _, other_ring, way, step, half in order:
            if other_ring == ring and step == 1:
                send(ring, way, step, half)
        pass_on(ring, rings[ring][1], 0, rings[ring][4])

    finish(second_c)
    begin_ring(2)
    work_out(start_of(2, k, z, 0), rings[2][4])
    finish(second_a)
    begin_ring(0)
    finish(second_b)
    begin_ring(1)
    work_out(start_of(0, k, x, 0), rings[0][4])
    work_out(start_of(1, k, y, 0), rings[1][4])
    done = 0
    for _, ring, way, step, half in order:
        axis, place, size, _, unit = rings[ring]
        pieces[ring, way, step, half].wait_recv()
        steps = size // 2
        if step + 1 < steps or (step + 1 == steps and half == (0 if way == 1 else 1)):
            send(ring, way, step + 1, half)
        at = shifted(place, -way * step, size)
        pass_on(ring, at, half, unit // 2)
        work_out(start_of(ring, k, at, half), unit // 2)
        to_other[done].wait_recv()
        work_out(*theirs[done])
        done += 1
    while done < len(to_other):
        to_other[done].wait_recv()
        work_out(*theirs[done])
        done += 1
    for copy in waiting + to_other:
        copy.wait_send()

    each = len(joins) // (ITERS * PARTS)

    sets = [joins[i * each : (i + 1) * each] for i in range(ITERS * PARTS)]

    def finish_totals(flows, tables, sums, mean):
        for _ in range(3):
            for flow in flows:
                next(flow)
        carry = None
        for part, flow in enumerate(flows):
            next(flow, None)
            table, base = tables[part]
            carry = moments(out, xt, table, base, sums[part], mean, acc, part, carry)
        return updated(mean, acc, carry, work)

    def flows_of(tables, sums, own):
        return [
            log_totals(*tables[part], sums[part], *own[part], z, y, k, x) for part in range(PARTS)
        ]

    tables = [(table1, part * (ROWS // PARTS)) for part in range(PARTS)]
    sums = (total1a, total1b)
    flows = flows_of(tables, sums, sets[:PARTS])
    for flow in flows:
        next(flow)
    mean, factor, weight = finish_totals(flows, tables, sums, mean_ref[...])
    mean2[...] = mean
    prepare(mean, factor, weight, main, rest, centre, offset)

    tables = [(table2a, 0), (table2b, 0)]
    sums = (total2a, total2b)
    flows = flows_of(tables, sums, sets[PARTS:])
    steps = NPTS // CHUNK // PARTS
    for part, flow in enumerate(flows):

        def again(i, carry):
            start = pl.multiple_of((part * steps + i) * CHUNK, CHUNK)
            density(
                xt[:, pl.ds(start, CHUNK)], tables[part][0], i * (CHUNK // D),
                main, rest, centre, offset,
            )
            return carry

        lax.fori_loop(0, steps, again, 0)
        next(flow)
    mean, factor, weight = finish_totals(flows, tables, sums, mean2[...])
    for part in range(PARTS):
        total2[part * (ROWS // PARTS) : (part + 1) * (ROWS // PARTS), :] = sums[part][...]
    own_density(total2, found, density_ref)
    new_mean_ref[...] = mean
    new_factor_ref[...] = factor
    new_weight_ref[...] = jnp.broadcast_to(weight, (1, D))


N_DIRECT = 2 * (NZ - 1) + 2 * (NX - 1) + 2 * (NY - 1)
N_RING = 2 * (NX - 1) + 2 * (NY - 1) + 2 * (NZ - 1)
N_OTHER = N_RING + 3


def shape(*dims):
    return jax.ShapeDtypeStruct(dims, F32)


def join_scratch():
    return [
        pltpu.VMEM((NC * NX - 1, PIECE, D), F32),
        pltpu.VMEM((PIECE, D), F32),
        pltpu.VMEM((NY - 1, PIECE, D), F32),
        pltpu.VMEM((PIECE, D), F32),
        pltpu.VMEM((NZ - 1, PIECE, D), F32),
        pltpu.SemaphoreType.DMA((2, N_LSE)),
    ]


def whole_step(counts, dests, points, mean, factor, weight):
    sem = pltpu.SemaphoreType.DMA
    return pl.pallas_call(
        step_kernel,
        out_shape=[shape(1, D), shape(D, D), shape(1, D), shape(RB * BR // D, D)],
        in_specs=[smem(), smem(), pl.BlockSpec(memory_space=pl.ANY)] + [vmem()] * 3,
        out_specs=[vmem()] * 4,
        scratch_shapes=[
            pltpu.SMEM((NZ * NSIDE,), jnp.int32),
            pltpu.VMEM((NB, BR, D), F32),
            pltpu.VMEM((NSIDE, BR, D), F32),
            pltpu.VMEM((NSIDE, BR, D), F32),
            pltpu.VMEM((NZ, BR, D), F32),
            pltpu.VMEM((NZ, BR, D), F32),
            pltpu.VMEM((NPTS, D), F32),
            pltpu.VMEM((D, NPTS), F32),
            pltpu.VMEM((ROWS, D), F32),
            *[pltpu.VMEM((ROWS // PARTS, D), F32)] * (3 * PARTS),
            pltpu.VMEM((ROWS, D), F32),
            pltpu.VMEM((1, D), F32),
            pltpu.VMEM((2 * D, 2 * D), BF16),
            pltpu.VMEM((D, 2 * D), BF16),
            pltpu.VMEM((D, D), F32),
            pltpu.VMEM((1, D), F32),
            pltpu.VMEM((2 * D, 2 * D), F32),
            pltpu.VMEM((D, 2 * D), F32),
            sem, sem((2, NSIDE)), sem((2, NZ)), sem((2, N_DIRECT)), sem((2, N_RING)),
            sem((2, N_OTHER)),
        ]
        + join_scratch() * (ITERS * PARTS),
        compiler_params=pltpu.CompilerParams(
            collective_id=0, has_side_effects=True, vmem_limit_bytes=VMEM_LIMIT
        ),
        name="whole_step",
    )(counts, dests, points, mean, factor, weight)


def per_device(points, block_counts, block_dest, means, factors, log_weights):
    new_mean, new_factor, new_weight, density_out = whole_step(
        block_counts, block_dest.T, points.reshape(NB, BR, D), means, factors[0],
        log_weights.reshape(1, 1),
    )
    return new_mean, new_factor[None], new_weight[0, :1], density_out.reshape(-1)


def solution(mesh):
    split = Mesh(mesh.devices.reshape(NZ, NY, NC, NX), DP_COMP)
    in_specs = (P(DP, None), P(), P(), P(DP_COMP, None), P(DP_COMP, None, None), P(DP_COMP))
    out_specs = (P(DP_COMP, None), P(DP_COMP, None, None), P(DP_COMP), P(DP))
    return jax.shard_map(
        per_device, mesh=split, in_specs=in_specs, out_specs=out_specs, check_vma=False
    )
```

```python
import math

import jax
import jax.numpy as jnp
from jax import lax
from jax.experimental import pallas as pl
from jax.experimental.pallas import tpu as pltpu
from jax.sharding import Mesh
from jax.sharding import PartitionSpec as P

D = 128
BR = 64
RB = 4
ITERS = 2
Z, Y, C, X = "dp_0", "dp_1", "dp_2", "comp"
DP = (Z, Y, C)
DP_COMP = (Z, Y, C, X)
NZ, NY, NC, NX = 8, 4, 2, 4
NPTS = NZ * NY * NC * NX * BR
ROWS = NPTS // D
NB = 16
NSIDE = NY * NC
GROUP = NSIDE * NX
PARTS = 2
PIECE = ROWS // (PARTS * NC * NX)
RA, RB_, RC = 24, 24, 16
BASE_B = NZ * NY * NC * NX * RA
BASE_C = BASE_B + NZ * NY * NC * NX * RB_
CHUNK = 2048
LOG_TWO_PI = math.log(2.0 * math.pi)
MESH = pl.DeviceIdType.MESH
F32, BF16 = jnp.float32, jnp.bfloat16
VMEM_LIMIT = 60 * 1024 * 1024


def vmem():
    return pl.BlockSpec(memory_space=pltpu.VMEM)


def smem():
    return pl.BlockSpec(memory_space=pltpu.SMEM)


def here():
    return lax.axis_index(Z), lax.axis_index(Y), lax.axis_index(C), lax.axis_index(X)


def shifted(place, step, size):
    return lax.rem(place + (step + size), size)


def split2(value):
    high = value.astype(BF16)
    return high, (value - high.astype(F32)).astype(BF16)


def split3(value):
    high = value.astype(BF16)
    rest = value - high.astype(F32)
    middle = rest.astype(BF16)
    return high, middle, (rest - middle.astype(F32)).astype(BF16)


def dot(a, b):
    return jnp.dot(a, b, preferred_element_type=F32)


def eye():
    return (
        lax.broadcasted_iota(jnp.int32, (D, D), 0) == lax.broadcasted_iota(jnp.int32, (D, D), 1)
    ).astype(F32)


def spread(row):
    return jnp.transpose(jnp.broadcast_to(row, (D, D)))


def moments(x_ref, xt_ref, table_ref, base, total_ref, mean, acc, part, carry):
    centre = spread(mean)
    groups = CHUNK // D
    steps = NPTS // CHUNK // PARTS

    def step(i, carry):
        first, count = carry
        start = pl.multiple_of(i * CHUNK, CHUNK)
        at = pl.multiple_of((i - part * steps) * groups, groups)
        share = jnp.exp(table_ref[pl.ds(base + at, groups), :] - total_ref[pl.ds(at, groups), :])
        wide = jnp.concatenate(
            [jnp.broadcast_to(share[g : g + 1, :], (D, D)) for g in range(groups)], axis=1
        )
        shift = xt_ref[:, pl.ds(start, CHUNK)] - jnp.concatenate([centre] * groups, axis=1)
        scaled = shift * wide
        for g in range(groups):
            first = first + scaled[:, g * D : (g + 1) * D]
        left = jnp.concatenate(split2(scaled), axis=0)
        right = jnp.concatenate(split2(x_ref[pl.ds(start, CHUNK), :] - mean), axis=1)
        acc[...] += dot(left, right)
        return first, count + share

    if part == 0:
        acc[...] = jnp.zeros_like(acc)
        carry = (jnp.zeros((D, D), F32), jnp.zeros((groups, D), F32))
    return lax.fori_loop(part * steps, (part + 1) * steps, step, carry)


def moment_sums(acc, carry):
    first, count = carry
    weight_sum = jnp.sum(jnp.sum(count, axis=0, keepdims=True), axis=1, keepdims=True)
    first_row = jnp.sum(jnp.transpose(first), axis=0, keepdims=True)
    second = acc[:D, :D] + acc[:D, D:] + acc[D:, :D] + acc[D:, D:]
    return weight_sum, first_row, second


def inverse_factor(covariance, work):
    work[:, :D] = covariance
    work[:, D:] = eye()
    place = lax.broadcasted_iota(jnp.int32, (8, D), 0)
    last = D // 8

    def wide(row):
        return jnp.broadcast_to(row, (8, D))

    for p in range(last):
        at = 8 * p
        left, right = work[at : at + 8, :D], work[at : at + 8, D:]
        if p == 0:
            columns = [wide(left[:, a : a + 1]) for a in range(8)]
        if p + 1 < last:
            left1, right1 = work[at + 8 : at + 16, :D], work[at + 8 : at + 16, D:]
            columns1 = [wide(left1[:, at + a : at + a + 1]) for a in range(8)]
            following = [wide(left1[:, at + 8 + b : at + 9 + b]) for b in range(8)]
        for a in range(8):
            pivot = wide(columns[a][a : a + 1, :])
            scale = lax.rsqrt(pivot)
            column = columns[a] * scale
            below = jnp.where(place > a, column, 0.0)
            row_left = wide(left[a : a + 1, :]) * scale
            row_right = wide(right[a : a + 1, :]) * scale
            left = jnp.where(place == a, row_left, left - below * row_left)
            right = jnp.where(place == a, row_right, right - below * row_right)
            across = [wide(column[b : b + 1, :]) for b in range(a + 1, 8)]
            for b in range(a + 1, 8):
                columns[b] = columns[b] - below * across[b - a - 1]
            if p + 1 < last:
                below1 = columns1[a] * scale
                left1 = left1 - below1 * row_left
                right1 = right1 - below1 * row_right
                for b in range(a + 1, 8):
                    columns1[b] = columns1[b] - below1 * across[b - a - 1]
                for b in range(8):
                    following[b] = following[b] - below1 * wide(below1[b : b + 1, :])
        work[at : at + 8, D:] = right
        if p + 1 < last:
            work[at + 8 : at + 16, :D] = left1
            work[at + 8 : at + 16, D:] = right1
            columns = following
        if p + 2 < last:
            h1, m1, l1 = [part.astype(F32) for part in split3(left)]
            both = jnp.concatenate([left, right], axis=1)
            h2, m2, l2 = [part.astype(F32) for part in split3(both)]
            one = jnp.concatenate([h1, h1, m1, h1, m1, l1], axis=0).astype(BF16)
            two = jnp.concatenate([h2, m2, h2, l2, m2, h2], axis=0).astype(BF16)
            change = lax.dot_general(
                one, two, (((0,), (0,)), ((), ())), preferred_element_type=F32
            )
            work[at + 16 :, :] = work[at + 16 :, :] - change[at + 16 :, :]
    return work[:, D:]


def offset_a(k, x, y=0, z=0):
    return (((k * NX + x) * NY + y) * NZ + z) * RA


def offset_b(k, y, z=0, x=0):
    return BASE_B + (((k * NY + y) * NZ + z) * NX + x) * RB_


def offset_c(k, z, x=0, y=0):
    return BASE_C + (((k * NZ + z) * NX + x) * NY + y) * RC


def remote(src, dst, ssem, rsem, target):
    return pltpu.make_async_remote_copy(
        src_ref=src, dst_ref=dst, send_sem=ssem, recv_sem=rsem,
        device_id=target, device_id_type=MESH,
    )


def side_at(side, step):
    t = shifted(side, step, NSIDE)
    return {Y: t // NC, C: lax.rem(t, NC)}


def enter(z, y, k, x):
    barrier = pltpu.get_barrier_semaphore()
    side = y * NC + k
    targets = [side_at(side, step) for step in range(1, NSIDE)]
    targets += [{Z: shifted(z, step, NZ)} for step in range(1, NZ)]
    targets += [{X: shifted(x, step, NX)} for step in range(1, NX)]
    targets += [{X: shifted(x, step, NX), C: 1 - k} for step in range(1, NX)]
    for target in targets:
        pl.semaphore_signal(barrier, inc=1, device_id=target, device_id_type=MESH)
    return barrier, len(targets)


def choose_blocks(counts, prefix, z, y, k, x):
    mine = (y * NC + k) * NX + x
    own = z * GROUP + mine

    def step(s, carry):
        before, first = carry
        prefix[s] = before
        return before + counts[s], first + (before <= own).astype(jnp.int32)

    _, first = lax.fori_loop(0, NZ * NSIDE, step, (jnp.int32(0), jnp.int32(-1)))
    start = prefix[z * NSIDE + y * NC + k]
    blocks = [
        jnp.minimum(jnp.bitwise_and(t * NX + x - start, GROUP - 1), NB - 1) for t in range(NSIDE)
    ]
    from_slot = [jnp.int32(0)] * NZ
    for t in range(NSIDE):
        sender = z * NSIDE + t
        j = jnp.bitwise_and(mine - prefix[sender], GROUP - 1)
        to_z = jnp.where(j < counts[sender], (prefix[sender] + j) // GROUP, NZ)
        from_slot = [jnp.where(to_z == i, t, from_slot[i]) for i in range(NZ)]
    return blocks, from_slot, first // NSIDE


def own_blocks(dests, counts, prefix, d):
    def step(s, carry):
        n, found = carry[0], carry[1:]
        at = jnp.int32(-1)
        for j in range(NB):
            at = jnp.where((dests[j, s] == d) & (j < counts[s]), j, at)
        number = prefix[s] + at
        here_too = at >= 0
        found = [jnp.where(here_too & (n == i), number, found[i]) for i in range(RB)]
        return (n + here_too.astype(jnp.int32), *found)

    return lax.fori_loop(0, NZ * NSIDE, step, (jnp.int32(0),) * (RB + 1))[1:]


def own_density(total, found, density_ref):
    lane = lax.broadcasted_iota(jnp.int32, (1, D), 1)
    line = jnp.zeros((1, D), F32)
    for i in range(RB):
        p = found[i]
        x = lax.rem(p, NX)
        k = lax.rem(lax.div(p, NX), NC)
        y = lax.rem(lax.div(p, NX * NC), NY)
        z = lax.div(p, GROUP)
        parts = (
            (0, offset_a(k, x, y, z), RA),
            (RA, offset_b(k, y, z, x), RB_),
            (RA + RB_, offset_c(k, z, x, y), RC),
        )
        for base, start, count in parts:
            row = lax.div(start, D)
            first = start - row * D
            to = (i % 2) * BR + base
            by = lax.rem(to - first + D, D)
            one = pltpu.roll(total[pl.ds(row, 1), :], by, 1)
            two = pltpu.roll(total[pl.ds(jnp.minimum(row + 1, ROWS - 1), 1), :], by, 1)
            value = jnp.where(lane - to + first < D, one, two)
            line = jnp.where((lane >= to) & (lane < to + count), value, line)
        if i % 2:
            density_ref[i // 2 : i // 2 + 1, :] = line / float(D)


def group_at(k, x, step):
    t = shifted(k * NX + x, step, NC * NX)
    return t, {C: t // NX, X: lax.rem(t, NX)}


def joined(parts):
    peak = parts[0]
    for part in parts[1:]:
        peak = jnp.maximum(peak, part)
    total = jnp.exp(parts[0] - peak)
    for part in parts[1:]:
        total = total + jnp.exp(part - peak)
    return peak + jnp.log(total)


def log_totals(table, base, out, rg, u, ry, w, rz, sem, z, y, k, x):
    members = NC * NX
    number = [0]

    def copy_to(src, dst, target):
        n = number[0]
        number[0] += 1
        copy = remote(src, dst, sem.at[0, n], sem.at[1, n], target)
        copy.start()
        return copy

    def piece(start, at):
        return pl.ds(pl.multiple_of(start + at * PIECE, 8), PIECE)

    mine = piece(0, k * NX + x)
    copies = []
    for step in range(1, members):
        at, target = group_at(k, x, step)
        copies.append(copy_to(table.at[piece(base, at)], rg.at[step - 1], target))
    yield
    for copy in copies:
        copy.wait()
    u[...] = joined([table[piece(base, k * NX + x), :]] + [rg[i] for i in range(members - 1)])
    copies = [
        copy_to(u, ry.at[step - 1], {Y: shifted(y, step, NY)}) for step in range(1, NY)
    ]
    yield
    for copy in copies:
        copy.wait()
    w[...] = joined([u[...]] + [ry[i] for i in range(NY - 1)])
    copies = [
        copy_to(w, rz.at[step - 1], {Z: shifted(z, step, NZ)}) for step in range(1, NZ)
    ]
    yield
    for copy in copies:
        copy.wait()
    out[mine, :] = joined([w[...]] + [rz[i] for i in range(NZ - 1)])
    copies = []
    for step in range(1, members):
        copies.append(copy_to(out.at[mine], out.at[mine], group_at(k, x, step)[1]))
    yield
    for copy in copies:
        copy.wait()


N_LSE = 2 * (NC * NX - 1) + (NY - 1) + (NZ - 1)


def prepare(mean, factor, weight, main, rest, centre, offset):
    high, middle, low = split3(jnp.transpose(factor))
    main[:D, :D] = high
    main[:D, D:] = high
    main[D:, :D] = middle
    main[D:, D:] = middle
    rest[:, :D] = high
    rest[:, D:] = low
    centre[...] = spread(mean)
    diagonal = jnp.sum(factor * eye(), axis=0, keepdims=True)
    offset[...] = jnp.broadcast_to(
        weight + jnp.sum(jnp.log(diagonal), axis=1, keepdims=True) - 0.5 * D * LOG_TWO_PI, (1, D)
    )


def density(turned, table, first_group, main, rest, centre, offset):
    groups = turned.shape[1] // D
    shift = turned - jnp.concatenate([centre[...]] * groups, axis=1)
    a, b, c = split3(shift)
    both = dot(main[...], jnp.concatenate([a, b], axis=0))
    value = both[:D] + both[D:] + dot(rest[...], jnp.concatenate([c, a], axis=0))
    total = jnp.sum(value * value, axis=0, keepdims=True)
    for g in range(groups):
        table[pl.ds(first_group + g, 1), :] = offset[...] - 0.5 * total[:, g * D : (g + 1) * D]


def updated(mean, acc, carry, work):
    weight_sum, first, second = moment_sums(acc, carry)
    counted = weight_sum + 1.0
    covariance = (second - spread(first) * (first / counted) + eye()) / counted
    covariance = 0.5 * (covariance + jnp.transpose(covariance))
    lower_inverse = inverse_factor(covariance, work)
    new_mean = mean + first / counted
    new_weight = jnp.log(counted / float(NPTS + NZ * NY * NC * NX))
    return new_mean, jnp.transpose(lower_inverse), new_weight


def step_kernel(
    counts, dests, points_ref, mean_ref, factor_ref, weight_ref,
    new_mean_ref, new_factor_ref, new_weight_ref, density_ref,
    prefix, points, slots, r1, s2, r2, out, xt, table1, table2a, table2b,
    total1a, total1b, total2a, total2b, total2, mean2,
    main, rest, centre, offset, acc, work, sem0, sem1, sem2, semg, sems, semk, *joins,
):
    z, y, k, x = here()
    side = y * NC + k
    load = pltpu.make_async_copy(points_ref, points, sem0)
    load.start()
    barrier, arrivals = enter(z, y, k, x)
    blocks, from_slot, own_slot = choose_blocks(counts, prefix, z, y, k, x)
    load.wait()
    for t in range(NSIDE):
        slots[t] = points[blocks[t]]
    pl.semaphore_wait(barrier, arrivals)

    copies = []
    for step in range(1, NSIDE):
        copies.append(
            remote(
                slots.at[shifted(side, step, NSIDE)], r1.at[side],
                sem1.at[0, step], sem1.at[1, step], side_at(side, step),
            )
        )
        copies[-1].start()
    r1[side] = slots[side]
    prepare(mean_ref[...], factor_ref[...], weight_ref[...], main, rest, centre, offset)
    for copy in copies:
        copy.wait()
    for t in range(NZ):
        s2[t] = r1[from_slot[t]]
    copies = []
    for step in range(1, NZ):
        t = shifted(z, step, NZ)
        copies.append(remote(s2.at[t], r2.at[z], sem2.at[0, step], sem2.at[1, step], {Z: t}))
        copies[-1].start()
    r2[z] = s2[z]
    found = own_blocks(dests, counts, prefix, z * NSIDE + side)
    for copy in copies:
        copy.wait()
    block = r2[own_slot]

    def rows(start, size):
        return out.at[pl.ds(pl.multiple_of(start, 8), size)]

    rows(offset_a(k, x, y, z), RA)[...] = block[:RA]
    rows(offset_b(k, y, z, x), RB_)[...] = block[RA : RA + RB_]
    rows(offset_c(k, z, x, y), RC)[...] = block[RA + RB_ :]

    number = [0]

    def spread_out(axis, place, size, start, count):
        part = rows(start, count)
        copies = []
        for step in range(1, size):
            n = number[0]
            number[0] += 1
            copies.append(
                remote(
                    part, part, semg.at[0, n], semg.at[1, n], {axis: shifted(place, step, size)}
                )
            )
            copies[-1].start()
        return copies

    def finish(copies):
        for copy in copies:
            copy.wait()

    first_b = spread_out(X, x, NX, offset_b(k, y, z, x), RB_)
    first_c = spread_out(Y, y, NY, offset_c(k, z, x, y), RC)
    first_a = spread_out(Z, z, NZ, offset_a(k, x, y, z), RA)
    finish(first_b)
    second_b = spread_out(Z, z, NZ, offset_b(k, y, z), NX * RB_)
    finish(first_c)
    second_c = spread_out(X, x, NX, offset_c(k, z, x), NY * RC)
    finish(first_a)
    second_a = spread_out(Y, y, NY, offset_a(k, x, y), NZ * RA)

    other = {C: 1 - k}
    rings = (
        (X, x, NX, offset_a, NY * NZ * RA),
        (Y, y, NY, offset_b, NZ * NX * RB_),
        (Z, z, NZ, offset_c, NX * NY * RC),
    )
    pieces = {}
    waiting = []
    to_other = []

    def start_of(ring, core, at, half):
        return rings[ring][3](core, at) + half * (rings[ring][4] // 2)

    def pass_on(ring, at, half, size):
        part = rows(start_of(ring, k, at, half), size)
        n = len(to_other)
        to_other.append(remote(part, part, semk.at[0, n], semk.at[1, n], other))
        to_other[-1].start()

    def work_out(start, size):
        unit = min(size, 3 * D)
        for i in range(0, size, unit):
            at = pl.multiple_of(start + i, D)
            turned = jnp.transpose(out[pl.ds(at, unit), :])
            xt[:, pl.ds(at, unit)] = turned
            density(turned, table1, at // D, main, rest, centre, offset)

    def send(ring, way, step, half):
        axis, place, size, _, unit = rings[ring]
        at = shifted(place, -way * (step - 1), size)
        part = rows(start_of(ring, k, at, half), unit // 2)
        n = len(waiting)
        copy = remote(
            part, part, sems.at[0, n], sems.at[1, n], {axis: shifted(place, way, size)}
        )
        copy.start()
        waiting.append(copy)
        pieces[ring, way, step, half] = copy

    order = []
    for ring in (0, 1, 2):
        steps = rings[ring][2] // 2
        begin, scale = (16.3, 4.2) if ring < 2 else (11.5, 1.5)
        for step in range(1, steps + 1):
            for late in (0, 1):
                if step == steps and late:
                    continue
                for way in (1, -1):
                    half = late if way == 1 else 1 - late
                    order.append((begin + scale * (2 * step + late - 1), ring, way, step, half))
    order.sort(key=lambda row: row[0])

    def begin_ring(ring):
        for _, other_ring, way, step, half in order:
            if other_ring == ring and step == 1:
                send(ring, way, step, half)
        pass_on(ring, rings[ring][1], 0, rings[ring][4])

    finish(second_c)
    begin_ring(2)
    work_out(start_of(2, k, z, 0), rings[2][4])
    finish(second_a)
    begin_ring(0)
    finish(second_b)
    begin_ring(1)
    work_out(start_of(0, k, x, 0), rings[0][4])
    work_out(start_of(1, k, y, 0), rings[1][4])
    groups = []
    for event in order:
        if groups and groups[-1][0][0] == event[0]:
            groups[-1].append(event)
        else:
            groups.append([event])

    def complete(events):
        units = []
        for _, ring, way, step, half in events:
            axis, place, size, _, unit = rings[ring]
            at = shifted(place, -way * step, size)
            if ring < 2:
                units.append((ring, at, half, unit // 2))
            elif way == 1 if step == size // 2 else half == (1 if way == 1 else 0):
                units.append((ring, at, 0, unit))
        return units

    def handle(core, units):
        for ring, at, half, size in units:
            work_out(start_of(ring, core, at, half), size)

    copies = list(to_other)
    units = [(ring, rings[ring][1], 0, rings[ring][4]) for ring in (2, 0, 1)]
    for events in groups + [[]]:
        first = len(to_other)
        for _, ring, way, step, half in events:
            axis, place, size, _, unit = rings[ring]
            pieces[ring, way, step, half].wait_recv()
            steps = size // 2
            if step + 1 < steps or (step + 1 == steps and half == (0 if way == 1 else 1)):
                send(ring, way, step + 1, half)
            pass_on(ring, shifted(place, -way * step, size), half, unit // 2)
        handle(k, complete(events))
        for copy in copies:
            copy.wait_recv()
        handle(1 - k, units)
        copies, units = to_other[first:], complete(events)
    for copy in waiting + to_other:
        copy.wait_send()

    each = len(joins) // (ITERS * PARTS)

    sets = [joins[i * each : (i + 1) * each] for i in range(ITERS * PARTS)]

    def finish_totals(flows, tables, sums, mean):
        for _ in range(3):
            for flow in flows:
                next(flow)
        carry = None
        for part, flow in enumerate(flows):
            next(flow, None)
            table, base = tables[part]
            carry = moments(out, xt, table, base, sums[part], mean, acc, part, carry)
        return updated(mean, acc, carry, work)

    def flows_of(tables, sums, own):
        return [
            log_totals(*tables[part], sums[part], *own[part], z, y, k, x) for part in range(PARTS)
        ]

    tables = [(table1, part * (ROWS // PARTS)) for part in range(PARTS)]
    sums = (total1a, total1b)
    flows = flows_of(tables, sums, sets[:PARTS])
    for flow in flows:
        next(flow)
    mean, factor, weight = finish_totals(flows, tables, sums, mean_ref[...])
    mean2[...] = mean
    prepare(mean, factor, weight, main, rest, centre, offset)

    tables = [(table2a, 0), (table2b, 0)]
    sums = (total2a, total2b)
    flows = flows_of(tables, sums, sets[PARTS:])
    steps = NPTS // CHUNK // PARTS
    for part, flow in enumerate(flows):

        def again(i, carry):
            start = pl.multiple_of((part * steps + i) * CHUNK, CHUNK)
            density(
                xt[:, pl.ds(start, CHUNK)], tables[part][0], i * (CHUNK // D),
                main, rest, centre, offset,
            )
            return carry

        lax.fori_loop(0, steps, again, 0)
        next(flow)
    mean, factor, weight = finish_totals(flows, tables, sums, mean2[...])
    for part in range(PARTS):
        total2[part * (ROWS // PARTS) : (part + 1) * (ROWS // PARTS), :] = sums[part][...]
    own_density(total2, found, density_ref)
    new_mean_ref[...] = mean
    new_factor_ref[...] = factor
    new_weight_ref[...] = jnp.broadcast_to(weight, (1, D))


N_DIRECT = 2 * (NZ - 1) + 2 * (NX - 1) + 2 * (NY - 1)
N_RING = 2 * (NX - 1) + 2 * (NY - 1) + 2 * (NZ - 1)
N_OTHER = N_RING + 3


def shape(*dims):
    return jax.ShapeDtypeStruct(dims, F32)


def join_scratch():
    return [
        pltpu.VMEM((NC * NX - 1, PIECE, D), F32),
        pltpu.VMEM((PIECE, D), F32),
        pltpu.VMEM((NY - 1, PIECE, D), F32),
        pltpu.VMEM((PIECE, D), F32),
        pltpu.VMEM((NZ - 1, PIECE, D), F32),
        pltpu.SemaphoreType.DMA((2, N_LSE)),
    ]


def whole_step(counts, dests, points, mean, factor, weight):
    sem = pltpu.SemaphoreType.DMA
    return pl.pallas_call(
        step_kernel,
        out_shape=[shape(1, D), shape(D, D), shape(1, D), shape(RB * BR // D, D)],
        in_specs=[smem(), smem(), pl.BlockSpec(memory_space=pl.ANY)] + [vmem()] * 3,
        out_specs=[vmem()] * 4,
        scratch_shapes=[
            pltpu.SMEM((NZ * NSIDE,), jnp.int32),
            pltpu.VMEM((NB, BR, D), F32),
            pltpu.VMEM((NSIDE, BR, D), F32),
            pltpu.VMEM((NSIDE, BR, D), F32),
            pltpu.VMEM((NZ, BR, D), F32),
            pltpu.VMEM((NZ, BR, D), F32),
            pltpu.VMEM((NPTS, D), F32),
            pltpu.VMEM((D, NPTS), F32),
            pltpu.VMEM((ROWS, D), F32),
            *[pltpu.VMEM((ROWS // PARTS, D), F32)] * (3 * PARTS),
            pltpu.VMEM((ROWS, D), F32),
            pltpu.VMEM((1, D), F32),
            pltpu.VMEM((2 * D, 2 * D), BF16),
            pltpu.VMEM((D, 2 * D), BF16),
            pltpu.VMEM((D, D), F32),
            pltpu.VMEM((1, D), F32),
            pltpu.VMEM((2 * D, 2 * D), F32),
            pltpu.VMEM((D, 2 * D), F32),
            sem, sem((2, NSIDE)), sem((2, NZ)), sem((2, N_DIRECT)), sem((2, N_RING)),
            sem((2, N_OTHER)),
        ]
        + join_scratch() * (ITERS * PARTS),
        compiler_params=pltpu.CompilerParams(
            collective_id=0, has_side_effects=True, vmem_limit_bytes=VMEM_LIMIT
        ),
        name="whole_step",
    )(counts, dests, points, mean, factor, weight)


def per_device(points, block_counts, block_dest, means, factors, log_weights):
    new_mean, new_factor, new_weight, density_out = whole_step(
        block_counts, block_dest.T, points.reshape(NB, BR, D), means, factors[0],
        log_weights.reshape(1, 1),
    )
    return new_mean, new_factor[None], new_weight[0, :1], density_out.reshape(-1)


def solution(mesh):
    split = Mesh(mesh.devices.reshape(NZ, NY, NC, NX), DP_COMP)
    in_specs = (P(DP, None), P(), P(), P(DP_COMP, None), P(DP_COMP, None, None), P(DP_COMP))
    out_specs = (P(DP_COMP, None), P(DP_COMP, None, None), P(DP_COMP), P(DP))
    return jax.shard_map(
        per_device, mesh=split, in_specs=in_specs, out_specs=out_specs, check_vma=False
    )
```
